128 devices in a mesh: subj: 4 (over y_lo, core), vox: 32 (over z, x, y_hi).
Axes of the slice: x: 4, y: 4 (y_hi: 2, y_lo: 2; y = y_hi * 2 + y_lo), z: 4, core: 2. Of those that a mesh axis runs over, the one named last changes fastest.
Arguments:
- series: bfloat16 [16, 256, 16384], P('subj', None, 'vox'), may hold values from -6 to 6
- offsets: int32 [16, 12], replicated, may hold values from 0 to 240
- selected: int32 [64], replicated, may hold values from 0 to 16383, as said below
Outputs:
- kernel: float32 [64, 192, 192], P('vox', 'subj')
The draws below stay inside these ranges and needn't reach their ends.
Inputs may be any that keep to these rules, and one draw needn't show every extreme that they name: `offsets`: each epoch lies inside its subject's run; epochs may intersect. `selected`: the ids are distinct.
All inputs are finite; a program needn't handle non-finite values.
Results may differ from the reference program's by a relative error of at most 0.00035.
Values may be sent and summed in bfloat16 or wider, within the bound.
No kernel may reach another device: no remote copies, remote signals or barrier semaphores. Data moves between devices by JAX's collectives and lax.ppermute only.
A program may use at most 128 MiB of HBM per device.

```python
import jax
import jax.numpy as jnp
from jax import lax

VOX = 16384
TR = 16
EP = 12
RUN_TR = 256
SUBJECTS = 16
SEL = 64


def draw_selected(key, part):
    first_key = jax.random.fold_in(key, 11)
    second_key = jax.random.fold_in(key, 12)
    middle = jax.random.permutation(first_key, VOX - 2)[:SEL - 2] + 1
    ends = jnp.array([0, VOX - 1], dtype=jnp.int32)
    joined = jnp.concatenate([ends, middle.astype(jnp.int32)])
    return jax.random.permutation(second_key, joined).astype(jnp.int32)


def plant(entries, stream_key, least, high):
    extent = entries.shape
    place = [jax.random.randint(jax.random.fold_in(stream_key, axis), (), 0, extent[axis]) for axis in range(len(extent))]
    entries = entries.at[tuple(place)].set(least)
    longest = extent.index(max(extent))
    place[longest] = (place[longest] + 1) % extent[longest]
    return entries.at[tuple(place)].set(high)


def block_levels(key, shape, cuts, smallest, top_value):
    def one(position, parts):
        steps = jax.random.uniform(jax.random.fold_in(jax.random.fold_in(key, 6), position), (parts,), jnp.float32, smallest / len(cuts), top_value / len(cuts))
        return jnp.repeat(jnp.exp(steps), shape[position] // parts).reshape((-1,) + (1,) * (len(shape) - position - 1))

    gain = one(*cuts[0])
    for cut in cuts[1:]:
        gain = gain * one(*cut)
    return gain


def bell_draw(key, dims, scale, reach, cuts=(), held_as=jnp.bfloat16):
    entries = scale * jax.random.normal(key, dims, jnp.float32)
    if cuts:
        entries = entries * block_levels(key, dims, cuts, -0.22, 0.18)
    return jnp.clip(entries, -reach, reach).astype(held_as)


def setup_inputs(seed: int = 0) -> dict:
    keys = jax.random.split(jax.random.key(seed), 4)
    return {
        "series": bell_draw(keys[0], (SUBJECTS, RUN_TR, VOX), 1.0, 6.0, ((0, 4), (2, 32))),
        "offsets": plant(jax.random.randint(keys[1], (SUBJECTS, EP), 0, RUN_TR - TR + 1), jax.random.fold_in(keys[1], 1), 0, RUN_TR - TR).astype(jnp.int32),
        "selected": draw_selected(jax.random.fold_in(keys[3], 71), 0),
    }


series_floor = 1.0
spread_floor = 0.05
shrink_factor = 0.9

def windows(block, starts):

    def subject_windows(subject_row, subject_offsets):
        return jax.vmap(lambda offset: lax.dynamic_slice_in_dim(subject_row, offset, TR, 0))(subject_offsets)
    return jax.vmap(subject_windows)(block, starts)

def standardize(values):
    centred = values - lax.optimization_barrier(jnp.mean(values, axis=2, keepdims=True))
    return centred / jnp.sqrt(lax.optimization_barrier(jnp.sum(centred * centred, axis=2, keepdims=True)) + series_floor)

def fisher_transform(correlation):
    shrunk = shrink_factor * correlation
    return 0.5 * jnp.log((1.0 + shrunk) / (1.0 - shrunk))

def scores(slab_std, voxel_std):
    correlation = jnp.einsum('setk,setv->ksev', slab_std, voxel_std, precision=lax.Precision.HIGHEST)
    fisher = fisher_transform(correlation)
    centred = fisher - lax.optimization_barrier(jnp.mean(fisher, axis=2, keepdims=True))
    variance = lax.optimization_barrier(jnp.mean(centred * centred, axis=2, keepdims=True))
    zscored = (centred / jnp.sqrt(variance + spread_floor)).astype(jnp.bfloat16)
    return zscored.reshape(zscored.shape[0], zscored.shape[1] * zscored.shape[2], zscored.shape[3])

def reference(series, offsets, selected):
    epochs = windows(series, offsets)
    voxel_std = standardize(epochs.astype(jnp.float32))
    slab_std = standardize(jnp.take(epochs, selected, axis=3).astype(jnp.float32))
    block_width = 8
    blocks = jnp.moveaxis(slab_std.reshape(slab_std.shape[:3] + (SEL // block_width, block_width)), 3, 0)

    def kernel_block(slab_block):
        zscored = scores(slab_block, voxel_std).astype(jnp.float32)
        return jnp.einsum('kev,kfv->kef', zscored, zscored, precision=lax.Precision.HIGHEST) * (1.0 / VOX)
    mapped = lax.map(kernel_block, blocks)
    return mapped.reshape(SEL, mapped.shape[2], mapped.shape[3])
```

```python
import jax
import jax.numpy as jnp
from jax import lax
from jax.experimental import pallas as pl
from jax.experimental.pallas import tpu as pltpu
from jax.sharding import PartitionSpec as P

TR = 16
EP = 12
GR = 4
SL = 4
SB = GR * SL
KL = 16
VOX = 16384
F32 = jnp.float32
BF16 = jnp.bfloat16
LINK = jnp.float16
series_floor = 1.0
spread_floor = 0.05
shrink_factor = 0.9


def iota(shape, dim):
    return lax.broadcasted_iota(jnp.int32, shape, dim)


def dot(a, b):
    return jnp.dot(a, b, preferred_element_type=F32)


def dot_nt(a, b):
    return lax.dot_general(a, b, (((1,), (1,)), ((), ())), preferred_element_type=F32)


def split(x):
    hi = x.astype(BF16)
    return hi, (x - hi.astype(F32)).astype(BF16)


def window_kernel(off_ref, sel_ref, series_ref, e_ref, t_ref, w_ref):
    j = lax.axis_index("subj")
    i = lax.axis_index("vox")
    width = series_ref.shape[2]
    lead = iota((TR, series_ref.shape[1]), 1) - iota((TR, series_ref.shape[1]), 0)
    for s in range(SL):
        for e in range(EP):
            chosen = lead == off_ref[j * SL + s, e]
            w_ref[e * TR : (e + 1) * TR, :] = jnp.where(chosen, 1.0, 0.0).astype(BF16)
        rows = dot(w_ref[...], series_ref[s]).astype(BF16)
        for e in range(EP):
            e_ref[e, s * TR : (s + 1) * TR, :] = rows[e * TR : (e + 1) * TR]
    row = iota((GR * KL, 128), 0)
    column = jnp.zeros((GR * KL, 128), jnp.int32)
    for r in range(GR):
        for k in range(KL):
            owner = (k // 4) * 8 + (j ^ r) * 2 + (k // 2) % 2
            column = jnp.where(row == r * KL + k, sel_ref[2 * owner + k % 2] - i * width, column)
    lane = iota((GR * KL, 128), 1)
    picker = jnp.concatenate(
        [jnp.where(column == lane + c, 1.0, 0.0).astype(BF16) for c in range(0, width, 128)], axis=1
    )
    t_ref[...] = dot_nt(picker, e_ref[...].reshape(EP * SL * TR, width)).astype(BF16)


def take_windows(series, offsets, selected):
    width = series.shape[2]
    return pl.pallas_call(
        window_kernel,
        out_shape=(
            jax.ShapeDtypeStruct((EP, SL * TR, width), BF16),
            jax.ShapeDtypeStruct((GR * KL, EP * SL * TR), BF16),
        ),
        in_specs=[
            pl.BlockSpec(memory_space=pltpu.SMEM),
            pl.BlockSpec(memory_space=pltpu.SMEM),
            pl.BlockSpec(memory_space=pltpu.VMEM),
        ],
        out_specs=(pl.BlockSpec(memory_space=pltpu.VMEM), pl.BlockSpec(memory_space=pltpu.VMEM)),
        scratch_shapes=[pltpu.VMEM((EP * TR, series.shape[1]), BF16)],
        name="windows",
    )(offsets, selected, series)


def kernel_kernel(e0, e1, e2, e3, s0, s1, s2, s3, o_ref, lh_ref, ll_ref, c_ref, n_ref, z_ref, g_ref):
    j = lax.axis_index("subj")
    epochs = (e0, e1, e2, e3)
    slabs = (s0, s1, s2, s3)
    width = e0.shape[2]
    deep = SB * TR
    chunk = SL * TR
    same = (iota((deep, deep), 0) // TR == iota((deep, deep), 1) // TR).astype(F32).astype(BF16)
    place = iota((SB, deep), 1)
    home = ((place // TR) % SL) * GR + ((place // chunk) ^ j)
    mine = iota((SB, deep), 0) == home
    gather = jnp.where(mine, 1.0, 0.0).astype(BF16)

    slab = jnp.concatenate(
        [
            jnp.concatenate([s[:, e * chunk : (e + 1) * chunk] for s in slabs], axis=1)
            for e in range(EP)
        ],
        axis=0,
    )
    centred = slab.astype(F32) - dot(slab, same) * (1.0 / TR)
    high, low = split(centred * centred)
    power = dot(high, same) + dot(low, same)
    slab_std = centred * (lax.rsqrt(power + series_floor) * shrink_factor)

    for e in range(EP):
        x = jnp.concatenate([p[e] for p in epochs], axis=0)
        xf = x.astype(F32)
        high, low = split(xf * xf)
        total = dot(gather, x)
        square = dot(gather, high) + dot(gather, low)
        n_ref[e] = lax.rsqrt(square - total * total * (1.0 / TR) + series_floor)
        for k in range(KL):
            line = jnp.where(mine, slab_std[e * KL + k : e * KL + k + 1, :], 0.0)
            lh, ll = split(line)
            lh_ref[k * SB : (k + 1) * SB, :] = lh
            ll_ref[k * SB : (k + 1) * SB, :] = ll
        c_ref[e] = dot(lh_ref[...], x) + dot(ll_ref[...], x)

    def pair(q, carry):
        for h in range(2):
            start = pl.multiple_of((q * 2 + h) * SB, SB)
            for c in range(0, width, 128):
                fisher = []
                for e in range(EP):
                    shrunk = c_ref[e, pl.ds(start, SB), c : c + 128] * n_ref[e, :, c : c + 128]
                    fisher.append(jnp.log(1.0 + shrunk) - jnp.log(1.0 - shrunk))
                mean = sum(fisher[1:], fisher[0]) * (1.0 / EP)
                fisher = [f - mean for f in fisher]
                spread = fisher[0] * fisher[0]
                for f in fisher[1:]:
                    spread = spread + f * f
                scale = lax.rsqrt(spread * (1.0 / EP) + 4.0 * spread_floor)
                for e in range(EP):
                    z_ref[h, e * SB : (e + 1) * SB, c : c + 128] = (fisher[e] * scale).astype(BF16)
            product = dot_nt(z_ref[h], z_ref[h])
            g_ref[h] = product[:, 0:128]
            g_ref[2, :, h * 64 : (h + 1) * 64] = product[:, 128 : EP * SB]
        base = (q // 2) * 8 + q % 2
        for r in range(GR):
            lines = pl.ds(r, EP * SL, stride=GR)
            both = jnp.concatenate([g_ref[n, lines, :] for n in range(3)], axis=0)
            o_ref[base + 2 * r] = both.astype(o_ref.dtype)
        return carry

    lax.fori_loop(0, KL // 2, pair, 0)


def partial_kernels(epochs, slabs, devices, dtype):
    width = epochs[0].shape[2]
    return pl.pallas_call(
        kernel_kernel,
        out_shape=jax.ShapeDtypeStruct((devices, 3 * EP * SL, 128), dtype),
        in_specs=[pl.BlockSpec(memory_space=pltpu.VMEM)] * (2 * GR),
        out_specs=pl.BlockSpec(memory_space=pltpu.VMEM),
        scratch_shapes=[
            pltpu.VMEM((KL * SB, SB * TR), BF16),
            pltpu.VMEM((KL * SB, SB * TR), BF16),
            pltpu.VMEM((EP, KL * SB, width), F32),
            pltpu.VMEM((EP, SB, width), F32),
            pltpu.VMEM((2, EP * SB, width), BF16),
            pltpu.VMEM((3, EP * SB, 128), F32),
        ],
        name="partial_kernels",
    )(*epochs, *slabs)


def order_kernel(y_ref, o_ref):
    rows = EP * SL
    cols = EP * SB
    source = iota((cols, cols), 0)
    target = (source % GR) * rows + ((source // GR) % SL) * EP + source // SB
    column = jnp.where(iota((cols, cols), 1) == target, 1.0, 0.0).astype(F32)
    source = iota((rows, rows), 1)
    line = jnp.where(iota((rows, rows), 0) == (source % SL) * EP + source // SL, 1.0, 0.0).astype(F32)
    exact = dict(precision=lax.Precision.HIGHEST, preferred_element_type=F32)
    for h in range(2):
        left = y_ref[h * rows : (h + 1) * rows, :]
        right = y_ref[2 * rows : 3 * rows, h * 64 : (h + 1) * 64]
        whole = jnp.concatenate([left, right], axis=1)
        o_ref[h] = jnp.dot(line, jnp.dot(whole, column, **exact), **exact) * (1.0 / VOX)


def in_order(tile):
    return pl.pallas_call(
        order_kernel,
        out_shape=jax.ShapeDtypeStruct((2, EP * SL, EP * SB), F32),
        in_specs=[pl.BlockSpec(memory_space=pltpu.VMEM)],
        out_specs=pl.BlockSpec(memory_space=pltpu.VMEM),
        name="in_order",
    )(tile)


def ring(step, size, stride, devices):
    def moved(n):
        place = (n // stride) % size
        return n + ((place + step) % size - place) * stride

    return [(n, moved(n)) for n in range(devices)]


def swapped(x, r):
    return lax.ppermute(x, "subj", [(n, n ^ r) for n in range(GR)])


def summed(x, size, stride, devices):
    parts = [lax.ppermute(x, "vox", ring(n, size, stride, devices)) for n in range(1, size)]
    return sum(parts, x)


def body(series, offsets, selected):
    devices = lax.axis_size("vox")
    own, picked = take_windows(series, offsets, selected)
    across = swapped(own, 2)
    beside = swapped(own, 1)
    beyond = swapped(across, 1)
    slab = summed(picked, 4, 8, devices)
    slab = summed(slab, 4, 2, devices)
    slab = summed(slab, 2, 1, devices)
    parts = [slab[r * KL : (r + 1) * KL] for r in range(GR)]
    parts = [parts[0]] + [swapped(parts[r], r) for r in range(1, GR)]
    tiles = partial_kernels((own, beside, across, beyond), parts, devices, F32)
    tiles = lax.all_to_all(tiles.astype(LINK), "vox", split_axis=0, concat_axis=0, tiled=True)
    tile = jnp.sum(tiles.astype(F32), axis=0)
    turn = [
        (j * devices + z * 8 + x * 2 + y, x * devices + z * 8 + j * 2 + y)
        for j in range(GR)
        for z in range(4)
        for x in range(4)
        for y in range(2)
    ]
    return in_order(lax.ppermute(tile, ("subj", "vox"), turn))


def solution(mesh):
    placed = (P("subj", None, "vox"), P(), P())
    return jax.shard_map(
        body, mesh=mesh, in_specs=placed, out_specs=P("vox", "subj", None), check_vma=False
    )
```

```python
import jax
import jax.numpy as jnp
from jax import lax
from jax.experimental import pallas as pl
from jax.experimental.pallas import tpu as pltpu
from jax.sharding import PartitionSpec as P


TR = 16
EP = 12
GR = 4
SL = 4
SB = GR * SL
KL = 16
VOX = 16384
F32 = jnp.float32
BF16 = jnp.bfloat16
LINK = jnp.float16
series_floor = 1.0
spread_floor = 0.05
shrink_factor = 0.9


def iota(shape, dim):
    return lax.broadcasted_iota(jnp.int32, shape, dim)


def dot(a, b):
    return jnp.dot(a, b, preferred_element_type=F32)


def dot_nt(a, b):
    return lax.dot_general(a, b, (((1,), (1,)), ((), ())), preferred_element_type=F32)


def split(x):
    hi = x.astype(BF16)
    return hi, (x - hi.astype(F32)).astype(BF16)


def window_kernel(off_ref, sel_ref, series_ref, e_ref, t_ref, w_ref):
    j = lax.axis_index("subj")
    i = lax.axis_index("vox")
    width = series_ref.shape[2]
    lead = iota((TR, series_ref.shape[1]), 1) - iota((TR, series_ref.shape[1]), 0)
    for s in range(SL):
        for e in range(EP):
            chosen = lead == off_ref[j * SL + s, e]
            w_ref[e * TR : (e + 1) * TR, :] = jnp.where(chosen, 1.0, 0.0).astype(BF16)
        rows = dot(w_ref[...], series_ref[s]).astype(BF16)
        for e in range(EP):
            e_ref[e, s * TR : (s + 1) * TR, :] = rows[e * TR : (e + 1) * TR]
    row = iota((GR * KL, 128), 0)
    column = jnp.zeros((GR * KL, 128), jnp.int32)
    for r in range(GR):
        for k in range(KL):
            owner = (k // 4) * 8 + (j ^ r) * 2 + (k // 2) % 2
            column = jnp.where(row == r * KL + k, sel_ref[2 * owner + k % 2] - i * width, column)
    lane = iota((GR * KL, 128), 1)
    picker = jnp.concatenate(
        [jnp.where(column == lane + c, 1.0, 0.0).astype(BF16) for c in range(0, width, 128)], axis=1
    )
    t_ref[...] = dot_nt(picker, e_ref[...].reshape(EP * SL * TR, width)).astype(BF16)


def take_windows(series, offsets, selected):
    width = series.shape[2]
    return pl.pallas_call(
        window_kernel,
        out_shape=(
            jax.ShapeDtypeStruct((EP, SL * TR, width), BF16),
            jax.ShapeDtypeStruct((GR * KL, EP * SL * TR), BF16),
        ),
        in_specs=[
            pl.BlockSpec(memory_space=pltpu.SMEM),
            pl.BlockSpec(memory_space=pltpu.SMEM),
            pl.BlockSpec(memory_space=pltpu.VMEM),
        ],
        out_specs=(pl.BlockSpec(memory_space=pltpu.VMEM), pl.BlockSpec(memory_space=pltpu.VMEM)),
        scratch_shapes=[pltpu.VMEM((EP * TR, series.shape[1]), BF16)],
        name="windows",
    )(offsets, selected, series)


def meeting(j, first, count):
    shape = (SB, count * SL * TR)
    place = iota(shape, 1)
    home = ((place // TR) % SL) * GR + ((place // (SL * TR) + first) ^ j)
    return iota(shape, 0) == home


def norm_kernel(first, e0, e1, n_ref):
    j = lax.axis_index("subj")
    gather = jnp.where(meeting(j, first, 2), 1.0, 0.0).astype(BF16)
    for e in range(EP):
        x = jnp.concatenate([e0[e], e1[e]], axis=0)
        xf = x.astype(F32)
        high, low = split(xf * xf)
        total = dot(gather, x)
        square = dot(gather, high) + dot(gather, low)
        n_ref[e] = square - total * total * (1.0 / TR)


def norms(e0, e1, first):
    return pl.pallas_call(
        lambda *refs: norm_kernel(first, *refs),
        out_shape=jax.ShapeDtypeStruct((EP, SB, e0.shape[2]), F32),
        in_specs=[pl.BlockSpec(memory_space=pltpu.VMEM)] * 2,
        out_specs=pl.BlockSpec(memory_space=pltpu.VMEM),
        name="norms",
    )(e0, e1)


def kernel_kernel(
    e0, e1, e2, e3, s0, s1, s2, s3, na, nb, o_ref, lh_ref, ll_ref, c_ref, n_ref, z_ref, g_ref
):
    j = lax.axis_index("subj")
    epochs = (e0, e1, e2, e3)
    slabs = (s0, s1, s2, s3)
    width = e0.shape[2]
    deep = SB * TR
    chunk = SL * TR
    same = (iota((deep, deep), 0) // TR == iota((deep, deep), 1) // TR).astype(F32).astype(BF16)
    mine = meeting(j, 0, GR)

    slab = jnp.concatenate(
        [
            jnp.concatenate([s[:, e * chunk : (e + 1) * chunk] for s in slabs], axis=1)
            for e in range(EP)
        ],
        axis=0,
    )
    centred = slab.astype(F32) - dot(slab, same) * (1.0 / TR)
    high, low = split(centred * centred)
    power = dot(high, same) + dot(low, same)
    slab_std = centred * (lax.rsqrt(power + series_floor) * shrink_factor)

    for e in range(EP):
        x = jnp.concatenate([p[e] for p in epochs], axis=0)
        n_ref[e] = lax.rsqrt(na[e] + nb[e] + series_floor)
        for k in range(KL):
            line = jnp.where(mine, slab_std[e * KL + k : e * KL + k + 1, :], 0.0)
            lh, ll = split(line)
            lh_ref[k * SB : (k + 1) * SB, :] = lh
            ll_ref[k * SB : (k + 1) * SB, :] = ll
        c_ref[e] = dot(lh_ref[...], x) + dot(ll_ref[...], x)

    def pair(q, carry):
        for h in range(2):
            start = pl.multiple_of((q * 2 + h) * SB, SB)
            for c in range(0, width, 128):
                fisher = []
                for e in range(EP):
                    shrunk = c_ref[e, pl.ds(start, SB), c : c + 128] * n_ref[e, :, c : c + 128]
                    fisher.append(jnp.log((1.0 + shrunk) / (1.0 - shrunk)))
                mean = sum(fisher[1:], fisher[0]) * (1.0 / EP)
                fisher = [f - mean for f in fisher]
                spread = fisher[0] * fisher[0]
                for f in fisher[1:]:
                    spread = spread + f * f
                scale = lax.rsqrt(spread * (1.0 / EP) + 4.0 * spread_floor)
                for e in range(EP):
                    z_ref[h, e * SB : (e + 1) * SB, c : c + 128] = (fisher[e] * scale).astype(BF16)
            product = dot_nt(z_ref[h], z_ref[h])
            g_ref[h] = product[:, 0:128]
            g_ref[2, :, h * 64 : (h + 1) * 64] = product[:, 128 : EP * SB]
        base = (q // 2) * 8 + q % 2
        for r in range(GR):
            lines = pl.ds(r, EP * SL, stride=GR)
            both = jnp.concatenate([g_ref[n, lines, :] for n in range(3)], axis=0)
            o_ref[base + 2 * r] = both.astype(o_ref.dtype)
        return carry

    lax.fori_loop(0, KL // 2, pair, 0)


def partial_kernels(epochs, slabs, powers, devices, dtype):
    width = epochs[0].shape[2]
    return pl.pallas_call(
        kernel_kernel,
        out_shape=jax.ShapeDtypeStruct((devices, 3 * EP * SL, 128), dtype),
        in_specs=[pl.BlockSpec(memory_space=pltpu.VMEM)] * (2 * GR + 2),
        out_specs=pl.BlockSpec(memory_space=pltpu.VMEM),
        scratch_shapes=[
            pltpu.VMEM((KL * SB, SB * TR), BF16),
            pltpu.VMEM((KL * SB, SB * TR), BF16),
            pltpu.VMEM((EP, KL * SB, width), F32),
            pltpu.VMEM((EP, SB, width), F32),
            pltpu.VMEM((2, EP * SB, width), BF16),
            pltpu.VMEM((3, EP * SB, 128), F32),
        ],
        name="partial_kernels",
    )(*epochs, *slabs, *powers)


def order_kernel(y_ref, o_ref):
    rows = EP * SL
    cols = EP * SB
    source = iota((cols, cols), 0)
    target = (source % GR) * rows + ((source // GR) % SL) * EP + source // SB
    column = jnp.where(iota((cols, cols), 1) == target, 1.0, 0.0).astype(BF16)
    for h in range(2):
        lines = []
        for s in range(SL):
            left = y_ref[pl.ds(h * rows + s, EP, stride=SL), :]
            right = y_ref[pl.ds(2 * rows + s, EP, stride=SL), :]
            lines.append(jnp.concatenate([left, right[:, h * 64 : (h + 1) * 64]], axis=1))
        whole = jnp.concatenate(lines, axis=0)
        high, _ = split(whole)
        middle, low = split(whole - high.astype(F32))
        o_ref[h] = (dot(high, column) + dot(middle, column) + dot(low, column)) * (1.0 / VOX)


def in_order(tile):
    return pl.pallas_call(
        order_kernel,
        out_shape=jax.ShapeDtypeStruct((2, EP * SL, EP * SB), F32),
        in_specs=[pl.BlockSpec(memory_space=pltpu.VMEM)],
        out_specs=pl.BlockSpec(memory_space=pltpu.VMEM),
        name="in_order",
    )(tile)


def ring(step, size, stride, devices):
    def moved(n):
        place = (n // stride) % size
        return n + ((place + step) % size - place) * stride

    return [(n, moved(n)) for n in range(devices)]


def swapped(x, r):
    return lax.ppermute(x, "subj", [(n, n ^ r) for n in range(GR)])


def summed(x, size, stride, devices):
    parts = [lax.ppermute(x, "vox", ring(n, size, stride, devices)) for n in range(1, size)]
    return sum(parts, x)


def body(series, offsets, selected):
    devices = lax.axis_size("vox")
    own, picked = take_windows(series, offsets, selected)
    across = swapped(own, 2)
    beside = swapped(own, 1)
    near = norms(own, beside, 0)
    slab = summed(picked, 4, 8, devices)
    slab = summed(slab, 4, 2, devices)
    slab = summed(slab, 2, 1, devices)
    beyond = swapped(across, 1)
    far = norms(across, beyond, 2)
    parts = [slab[r * KL : (r + 1) * KL] for r in range(GR)]
    parts = [parts[0]] + [swapped(parts[r], r) for r in range(1, GR)]
    tiles = partial_kernels((own, beside, across, beyond), parts, (near, far), devices, F32)
    tiles = lax.all_to_all(tiles.astype(LINK), "vox", split_axis=0, concat_axis=0, tiled=True)
    tile = jnp.sum(tiles.astype(F32), axis=0)
    turn = [
        (j * devices + z * 8 + x * 2 + y, x * devices + z * 8 + j * 2 + y)
        for j in range(GR)
        for z in range(4)
        for x in range(4)
        for y in range(2)
    ]
    return in_order(lax.ppermute(tile, ("subj", "vox"), turn))


def solution(mesh):
    placed = (P("subj", None, "vox"), P(), P())
    return jax.shard_map(
        body, mesh=mesh, in_specs=placed, out_specs=P("vox", "subj", None), check_vma=False
    )
```

```python
import jax
import jax.numpy as jnp
from jax import lax
from jax.experimental import pallas as pl
from jax.experimental.pallas import tpu as pltpu
from jax.sharding import PartitionSpec as P


TR = 16
EP = 12
GR = 4
SL = 4
SB = GR * SL
KL = 16
VOX = 16384
F32 = jnp.float32
BF16 = jnp.bfloat16
LINK = jnp.float16
series_floor = 1.0
spread_floor = 0.05
shrink_factor = 0.9


def near(x):
    return pltpu.with_memory_space_constraint(x, pltpu.VMEM)


def iota(shape, dim):
    return lax.broadcasted_iota(jnp.int32, shape, dim)


def dot(a, b):
    return jnp.dot(a, b, preferred_element_type=F32)


def dot_nt(a, b):
    return lax.dot_general(a, b, (((1,), (1,)), ((), ())), preferred_element_type=F32)


def split(x):
    hi = x.astype(BF16)
    return hi, (x - hi.astype(F32)).astype(BF16)


def window_kernel(off_ref, sel_ref, series_ref, e_ref, t_ref, w_ref):
    j = lax.axis_index("subj")
    i = lax.axis_index("vox")
    width = series_ref.shape[2]
    lead = iota((TR, series_ref.shape[1]), 1) - iota((TR, series_ref.shape[1]), 0)
    for s in range(SL):
        for e in range(EP):
            chosen = lead == off_ref[j * SL + s, e]
            w_ref[e * TR : (e + 1) * TR, :] = jnp.where(chosen, 1.0, 0.0).astype(BF16)
        rows = dot(w_ref[...], series_ref[s]).astype(BF16)
        for e in range(EP):
            e_ref[e, s * TR : (s + 1) * TR, :] = rows[e * TR : (e + 1) * TR]
    row = iota((GR * KL, 128), 0)
    column = jnp.zeros((GR * KL, 128), jnp.int32)
    for r in range(GR):
        for k in range(KL):
            owner = (k // 4) * 8 + (j ^ r) * 2 + (k // 2) % 2
            column = jnp.where(row == r * KL + k, sel_ref[2 * owner + k % 2] - i * width, column)
    lane = iota((GR * KL, 128), 1)
    picker = jnp.concatenate(
        [jnp.where(column == lane + c, 1.0, 0.0).astype(BF16) for c in range(0, width, 128)], axis=1
    )
    t_ref[...] = dot_nt(picker, e_ref[...].reshape(EP * SL * TR, width)).astype(BF16)


def take_windows(series, offsets, selected):
    width = series.shape[2]
    return pl.pallas_call(
        window_kernel,
        out_shape=(
            pltpu.VMEM((EP, SL * TR, width), BF16),
            pltpu.VMEM((GR * KL, EP * SL * TR), BF16),
        ),
        in_specs=[
            pl.BlockSpec(memory_space=pltpu.SMEM),
            pl.BlockSpec(memory_space=pltpu.SMEM),
            pl.BlockSpec(memory_space=pltpu.VMEM),
        ],
        out_specs=(pl.BlockSpec(memory_space=pltpu.VMEM), pl.BlockSpec(memory_space=pltpu.VMEM)),
        scratch_shapes=[pltpu.VMEM((EP * TR, series.shape[1]), BF16)],
        compiler_params=pltpu.CompilerParams(vmem_limit_bytes=8 << 20),
        name="windows",
    )(offsets, selected, series)


def meeting(j, first, count):
    shape = (SB, count * SL * TR)
    place = iota(shape, 1)
    home = ((place // TR) % SL) * GR + ((place // (SL * TR) + first) ^ j)
    return iota(shape, 0) == home


def norm_kernel(first, e0, e1, n_ref):
    j = lax.axis_index("subj")
    gather = jnp.where(meeting(j, first, 2), 1.0, 0.0).astype(BF16)
    for e in range(EP):
        x = jnp.concatenate([e0[e], e1[e]], axis=0)
        xf = x.astype(F32)
        high, low = split(xf * xf)
        total = dot(gather, x)
        square = dot(gather, high) + dot(gather, low)
        n_ref[e] = square - total * total * (1.0 / TR)


def norms(e0, e1, first):
    return pl.pallas_call(
        lambda *refs: norm_kernel(first, *refs),
        out_shape=pltpu.VMEM((EP, SB, e0.shape[2]), F32),
        in_specs=[pl.BlockSpec(memory_space=pltpu.VMEM)] * 2,
        out_specs=pl.BlockSpec(memory_space=pltpu.VMEM),
        compiler_params=pltpu.CompilerParams(vmem_limit_bytes=4 << 20),
        name="norms",
    )(near(e0), near(e1))


def kernel_kernel(
    e0, e1, e2, e3, s0, s1, s2, s3, na, nb, o_ref, lh_ref, ll_ref, c_ref, n_ref, z_ref, g_ref
):
    j = lax.axis_index("subj")
    epochs = (e0, e1, e2, e3)
    slabs = (s0, s1, s2, s3)
    width = e0.shape[2]
    deep = SB * TR
    chunk = SL * TR
    same = (iota((deep, deep), 0) // TR == iota((deep, deep), 1) // TR).astype(F32).astype(BF16)
    mine = meeting(j, 0, GR)

    slab = jnp.concatenate(
        [
            jnp.concatenate([s[:, e * chunk : (e + 1) * chunk] for s in slabs], axis=1)
            for e in range(EP)
        ],
        axis=0,
    )
    centred = slab.astype(F32) - dot(slab, same) * (1.0 / TR)
    high, low = split(centred * centred)
    power = dot(high, same) + dot(low, same)
    slab_std = centred * (lax.rsqrt(power + series_floor) * shrink_factor)

    for e in range(EP):
        x = jnp.concatenate([p[e] for p in epochs], axis=0)
        n_ref[e] = lax.rsqrt(na[e] + nb[e] + series_floor)
        for k in range(KL):
            line = jnp.where(mine, slab_std[e * KL + k : e * KL + k + 1, :], 0.0)
            lh, ll = split(line)
            lh_ref[k * SB : (k + 1) * SB, :] = lh
            ll_ref[k * SB : (k + 1) * SB, :] = ll
        c_ref[e] = dot(lh_ref[...], x) + dot(ll_ref[...], x)

    def pair(q, carry):
        for h in range(2):
            start = pl.multiple_of((q * 2 + h) * SB, SB)
            for c in range(0, width, 128):
                fisher = []
                for e in range(EP):
                    shrunk = c_ref[e, pl.ds(start, SB), c : c + 128] * n_ref[e, :, c : c + 128]
                    fisher.append(jnp.log((1.0 + shrunk) / (1.0 - shrunk)))
                mean = sum(fisher[1:], fisher[0]) * (1.0 / EP)
                fisher = [f - mean for f in fisher]
                spread = fisher[0] * fisher[0]
                for f in fisher[1:]:
                    spread = spread + f * f
                scale = lax.rsqrt(spread * (1.0 / EP) + 4.0 * spread_floor)
                for e in range(EP):
                    z_ref[h, e * SB : (e + 1) * SB, c : c + 128] = (fisher[e] * scale).astype(BF16)
            product = dot_nt(z_ref[h], z_ref[h])
            g_ref[h] = product[:, 0:128]
            g_ref[2, :, h * 64 : (h + 1) * 64] = product[:, 128 : EP * SB]
        base = (q // 2) * 8 + q % 2
        for r in range(GR):
            lines = pl.ds(r, EP * SL, stride=GR)
            both = jnp.concatenate([g_ref[n, lines, :] for n in range(3)], axis=0)
            o_ref[base + 2 * r] = both.astype(o_ref.dtype)
        return carry

    lax.fori_loop(0, KL // 2, pair, 0)


def partial_kernels(epochs, slabs, powers, devices, dtype):
    width = epochs[0].shape[2]
    return pl.pallas_call(
        kernel_kernel,
        out_shape=pltpu.VMEM((devices, 3 * EP * SL, 128), dtype),
        in_specs=[pl.BlockSpec(memory_space=pltpu.VMEM)] * (2 * GR + 2),
        out_specs=pl.BlockSpec(memory_space=pltpu.VMEM),
        scratch_shapes=[
            pltpu.VMEM((KL * SB, SB * TR), BF16),
            pltpu.VMEM((KL * SB, SB * TR), BF16),
            pltpu.VMEM((EP, KL * SB, width), F32),
            pltpu.VMEM((EP, SB, width), F32),
            pltpu.VMEM((2, EP * SB, width), BF16),
            pltpu.VMEM((3, EP * SB, 128), F32),
        ],
        compiler_params=pltpu.CompilerParams(vmem_limit_bytes=20 << 20),
        name="partial_kernels",
    )(*map(near, (*epochs, *slabs, *powers)))


def order_kernel(y_ref, o_ref):
    rows = EP * SL
    cols = EP * SB
    source = iota((cols, cols), 0)
    target = (source % GR) * rows + ((source // GR) % SL) * EP + source // SB
    column = jnp.where(iota((cols, cols), 1) == target, 1.0, 0.0).astype(BF16)
    for h in range(2):
        lines = []
        for s in range(SL):
            left = y_ref[pl.ds(h * rows + s, EP, stride=SL), :]
            right = y_ref[pl.ds(2 * rows + s, EP, stride=SL), :]
            lines.append(jnp.concatenate([left, right[:, h * 64 : (h + 1) * 64]], axis=1))
        whole = jnp.concatenate(lines, axis=0)
        high, _ = split(whole)
        middle, low = split(whole - high.astype(F32))
        o_ref[h] = (dot(high, column) + dot(middle, column) + dot(low, column)) * (1.0 / VOX)


def in_order(tile):
    return pl.pallas_call(
        order_kernel,
        out_shape=jax.ShapeDtypeStruct((2, EP * SL, EP * SB), F32),
        in_specs=[pl.BlockSpec(memory_space=pltpu.VMEM)],
        out_specs=pl.BlockSpec(memory_space=pltpu.VMEM),
        compiler_params=pltpu.CompilerParams(vmem_limit_bytes=4 << 20),
        name="in_order",
    )(near(tile))


def ring(step, size, stride, devices):
    def moved(n):
        place = (n // stride) % size
        return n + ((place + step) % size - place) * stride

    return [(n, moved(n)) for n in range(devices)]


def swapped(x, r):
    return lax.ppermute(x, "subj", [(n, n ^ r) for n in range(GR)])


def summed(x, size, stride, devices):
    parts = [lax.ppermute(x, "vox", ring(n, size, stride, devices)) for n in range(1, size)]
    return sum(parts, x)


def body(series, offsets, selected):
    devices = lax.axis_size("vox")
    own, picked = take_windows(series, offsets, selected)
    across = swapped(own, 2)
    beside = swapped(own, 1)
    first = norms(own, beside, 0)
    slab = summed(picked, 4, 8, devices)
    slab = summed(slab, 4, 2, devices)
    slab = summed(slab, 2, 1, devices)
    beyond = swapped(across, 1)
    second = norms(across, beyond, 2)
    parts = [slab[r * KL : (r + 1) * KL] for r in range(GR)]
    parts = [parts[0]] + [swapped(parts[r], r) for r in range(1, GR)]
    tiles = partial_kernels((own, beside, across, beyond), parts, (first, second), devices, F32)
    tiles = lax.all_to_all(tiles.astype(LINK), "vox", split_axis=0, concat_axis=0, tiled=True)
    tile = jnp.sum(tiles.astype(F32), axis=0)
    turn = [
        (j * devices + z * 8 + x * 2 + y, x * devices + z * 8 + j * 2 + y)
        for j in range(GR)
        for z in range(4)
        for x in range(4)
        for y in range(2)
    ]
    return in_order(lax.ppermute(tile, ("subj", "vox"), turn))


def solution(mesh):
    placed = (P("subj", None, "vox"), P(), P())
    return jax.shard_map(
        body, mesh=mesh, in_specs=placed, out_specs=P("vox", "subj", None), check_vma=False
    )
```

```python
import jax
import jax.numpy as jnp
from jax import lax
from jax.experimental import pallas as pl
from jax.experimental.pallas import tpu as pltpu
from jax.sharding import PartitionSpec as P


TR = 16
EP = 12
GR = 4
SL = 4
SB = GR * SL
KL = 16
HALF = EP * SB // 3
BLOCKS = ((0, 0), (0, 1), (0, 2), (1, 1), (1, 2), (2, 2))
QUARTER = len(BLOCKS) * HALF // GR
VOX = 16384
F32 = jnp.float32
BF16 = jnp.bfloat16
LINK = jnp.float16
series_floor = 1.0
spread_floor = 0.05
shrink_factor = 0.9


def near(x):
    return pltpu.with_memory_space_constraint(x, pltpu.VMEM)


def iota(shape, dim):
    return lax.broadcasted_iota(jnp.int32, shape, dim)


def dot(a, b):
    return jnp.dot(a, b, preferred_element_type=F32)


def dot_nt(a, b):
    return lax.dot_general(a, b, (((1,), (1,)), ((), ())), preferred_element_type=F32)


def split(x):
    hi = x.astype(BF16)
    return hi, (x - hi.astype(F32)).astype(BF16)


def window_kernel(off_ref, sel_ref, series_ref, e_ref, t_ref, w_ref):
    j = lax.axis_index("subj")
    i = lax.axis_index("vox")
    width = series_ref.shape[2]
    lead = iota((TR, series_ref.shape[1]), 1) - iota((TR, series_ref.shape[1]), 0)
    for s in range(SL):
        for e in range(EP):
            chosen = lead == off_ref[j * SL + s, e]
            w_ref[e * TR : (e + 1) * TR, :] = jnp.where(chosen, 1.0, 0.0).astype(BF16)
        rows = dot(w_ref[...], series_ref[s]).astype(BF16)
        for e in range(EP):
            e_ref[e, s * TR : (s + 1) * TR, :] = rows[e * TR : (e + 1) * TR]
    row = iota((GR * KL, 128), 0)
    column = jnp.zeros((GR * KL, 128), jnp.int32)
    for r in range(GR):
        for k in range(KL):
            owner = (k // 4) * 8 + (j ^ r) * 2 + (k // 2) % 2
            column = jnp.where(row == r * KL + k, sel_ref[2 * owner + k % 2] - i * width, column)
    lane = iota((GR * KL, 128), 1)
    picker = jnp.concatenate(
        [jnp.where(column == lane + c, 1.0, 0.0).astype(BF16) for c in range(0, width, 128)], axis=1
    )
    t_ref[...] = dot_nt(picker, e_ref[...].reshape(EP * SL * TR, width)).astype(BF16)


def take_windows(series, offsets, selected):
    width = series.shape[2]
    return pl.pallas_call(
        window_kernel,
        out_shape=(
            pltpu.VMEM((EP, SL * TR, width), BF16),
            pltpu.VMEM((GR * KL, EP * SL * TR), BF16),
        ),
        in_specs=[
            pl.BlockSpec(memory_space=pltpu.SMEM),
            pl.BlockSpec(memory_space=pltpu.SMEM),
            pl.BlockSpec(memory_space=pltpu.VMEM),
        ],
        out_specs=(pl.BlockSpec(memory_space=pltpu.VMEM), pl.BlockSpec(memory_space=pltpu.VMEM)),
        scratch_shapes=[pltpu.VMEM((EP * TR, series.shape[1]), BF16)],
        compiler_params=pltpu.CompilerParams(vmem_limit_bytes=8 << 20),
        name="windows",
    )(
        pltpu.with_memory_space_constraint(offsets, pltpu.HBM),
        pltpu.with_memory_space_constraint(selected, pltpu.HBM),
        pltpu.with_memory_space_constraint(series, pltpu.HBM),
    )


def meeting(j, first, count):
    shape = (SB, count * SL * TR)
    place = iota(shape, 1)
    home = ((place // TR) % SL) * GR + ((place // (SL * TR) + first) ^ j)
    return iota(shape, 0) == home


def norm_kernel(first, e0, e1, n_ref):
    j = lax.axis_index("subj")
    gather = jnp.where(meeting(j, first, 2), 1.0, 0.0).astype(BF16)
    for e in range(EP):
        x = jnp.concatenate([e0[e], e1[e]], axis=0)
        xf = x.astype(F32)
        high, low = split(xf * xf)
        total = dot(gather, x)
        square = dot(gather, high) + dot(gather, low)
        n_ref[e] = square - total * total * (1.0 / TR)


def norms(e0, e1, first):
    return pl.pallas_call(
        lambda *refs: norm_kernel(first, *refs),
        out_shape=pltpu.VMEM((EP, SB, e0.shape[2]), F32),
        in_specs=[pl.BlockSpec(memory_space=pltpu.VMEM)] * 2,
        out_specs=pl.BlockSpec(memory_space=pltpu.VMEM),
        compiler_params=pltpu.CompilerParams(vmem_limit_bytes=4 << 20),
        name="norms",
    )(near(e0), near(e1))


def kernel_kernel(
    e0, e1, e2, e3, s0, s1, s2, s3, na, nb, o_ref, lh_ref, ll_ref, c_ref, n_ref, z_ref
):
    j = lax.axis_index("subj")
    epochs = (e0, e1, e2, e3)
    slabs = (s0, s1, s2, s3)
    width = e0.shape[2]
    deep = SB * TR
    chunk = SL * TR
    same = (iota((deep, deep), 0) // TR == iota((deep, deep), 1) // TR).astype(F32).astype(BF16)
    mine = meeting(j, 0, GR)

    slab = jnp.concatenate(
        [
            jnp.concatenate([s[:, e * chunk : (e + 1) * chunk] for s in slabs], axis=1)
            for e in range(EP)
        ],
        axis=0,
    )
    centred = slab.astype(F32) - dot(slab, same) * (1.0 / TR)
    high, low = split(centred * centred)
    power = dot(high, same) + dot(low, same)
    slab_std = centred * (lax.rsqrt(power + series_floor) * shrink_factor)

    for e in range(EP):
        x = jnp.concatenate([p[e] for p in epochs], axis=0)
        n_ref[e] = lax.rsqrt(na[e] + nb[e] + series_floor)
        for k in range(KL):
            line = jnp.where(mine, slab_std[e * KL + k : e * KL + k + 1, :], 0.0)
            lh, ll = split(line)
            lh_ref[k * SB : (k + 1) * SB, :] = lh
            ll_ref[k * SB : (k + 1) * SB, :] = ll
        c_ref[e] = dot(lh_ref[...], x) + dot(ll_ref[...], x)

    def pair(q, carry):
        base = (q // 2) * 8 + q % 2
        for h in range(2):
            start = pl.multiple_of((q * 2 + h) * SB, SB)
            for c in range(0, width, 128):
                fisher = []
                for e in range(EP):
                    shrunk = c_ref[e, pl.ds(start, SB), c : c + 128] * n_ref[e, :, c : c + 128]
                    fisher.append(jnp.log((1.0 + shrunk) / (1.0 - shrunk)))
                mean = sum(fisher[1:], fisher[0]) * (1.0 / EP)
                fisher = [f - mean for f in fisher]
                spread = fisher[0] * fisher[0]
                for f in fisher[1:]:
                    spread = spread + f * f
                scale = lax.rsqrt(spread * (1.0 / EP) + 4.0 * spread_floor)
                for e in range(EP):
                    z_ref[h, e * SB : (e + 1) * SB, c : c + 128] = (fisher[e] * scale).astype(BF16)
            for n, (low, high) in enumerate(BLOCKS):
                left = z_ref[h, low * HALF : (low + 1) * HALF, :]
                tile = dot_nt(left, z_ref[h, high * HALF : (high + 1) * HALF, :])
                for first in range(0, HALF, HALF // 2):
                    at, line = divmod(n * HALF + first, QUARTER)
                    part = tile[first : first + HALF // 2]
                    o_ref[base + 2 * at, line : line + HALF // 2, h * HALF : (h + 1) * HALF] = part
        return carry

    lax.fori_loop(0, KL // 2, pair, 0)


def partial_kernels(epochs, slabs, powers, devices, dtype):
    width = epochs[0].shape[2]
    return pl.pallas_call(
        kernel_kernel,
        out_shape=pltpu.VMEM((devices, QUARTER, 2 * HALF), dtype),
        in_specs=[pl.BlockSpec(memory_space=pltpu.VMEM)] * (2 * GR + 2),
        out_specs=pl.BlockSpec(memory_space=pltpu.VMEM),
        scratch_shapes=[
            pltpu.VMEM((KL * SB, SB * TR), BF16),
            pltpu.VMEM((KL * SB, SB * TR), BF16),
            pltpu.VMEM((EP, KL * SB, width), F32),
            pltpu.VMEM((EP, SB, width), F32),
            pltpu.VMEM((2, EP * SB, width), BF16),
        ],
        compiler_params=pltpu.CompilerParams(vmem_limit_bytes=20 << 20),
        name="partial_kernels",
    )(*map(near, (*epochs, *slabs, *powers)))


def order_kernel(y0, y1, y2, y3, o_ref, b_ref, k_ref):
    j = lax.axis_index("subj")
    for r, y in enumerate((y0, y1, y2, y3)):
        b_ref[pl.ds(pl.multiple_of((j ^ r) * QUARTER, QUARTER), QUARTER), :] = y[...]
    for n, (low, high) in enumerate(BLOCKS):
        tile = b_ref[n * HALF : (n + 1) * HALF, :]
        mirrored = tile.T
        for h in range(2):
            block = tile[:, h * HALF : (h + 1) * HALF]
            at = (high % 2) * HALF
            k_ref[h, high // 2, low * HALF : (low + 1) * HALF, at : at + HALF] = block
            if low != high:
                block = mirrored[h * HALF : (h + 1) * HALF]
                at = (low % 2) * HALF
                k_ref[h, low // 2, high * HALF : (high + 1) * HALF, at : at + HALF] = block
    cols = EP * SB
    source = iota((cols, cols), 0)
    target = (source % GR) * (EP * SL) + ((source // GR) % SL) * EP + source // SB
    column = jnp.where(iota((cols, cols), 1) == target, 1.0, 0.0).astype(BF16)
    for h in range(2):
        lines = []
        for s in range(SL):
            own = pl.ds(s * GR + j, EP, stride=SB)
            lines.append(jnp.concatenate([k_ref[h, 0, own, :], k_ref[h, 1, own, :][:, 0:HALF]], axis=1))
        whole = jnp.concatenate(lines, axis=0)
        high, _ = split(whole)
        middle, low = split(whole - high.astype(F32))
        o_ref[h] = (dot(high, column) + dot(middle, column) + dot(low, column)) * (1.0 / VOX)


def in_order(tiles):
    return pl.pallas_call(
        order_kernel,
        out_shape=jax.ShapeDtypeStruct((2, EP * SL, EP * SB), F32),
        in_specs=[pl.BlockSpec(memory_space=pltpu.VMEM)] * GR,
        out_specs=pl.BlockSpec(memory_space=pltpu.VMEM),
        scratch_shapes=[
            pltpu.VMEM((len(BLOCKS) * HALF, 2 * HALF), F32),
            pltpu.VMEM((2, 2, EP * SB, 2 * HALF), F32),
        ],
        compiler_params=pltpu.CompilerParams(vmem_limit_bytes=4 << 20),
        name="in_order",
    )(*map(near, tiles))


def ring(step, size, stride, devices):
    def moved(n):
        place = (n // stride) % size
        return n + ((place + step) % size - place) * stride

    return [(n, moved(n)) for n in range(devices)]


def swapped(x, r):
    return lax.ppermute(x, "subj", [(n, n ^ r) for n in range(GR)])


def summed(x, size, stride, devices):
    parts = [lax.ppermute(x, "vox", ring(n, size, stride, devices)) for n in range(1, size)]
    return sum(parts, x)


def body(series, offsets, selected):
    devices = lax.axis_size("vox")
    own, picked = take_windows(series, offsets, selected)
    across = swapped(own, 2)
    beside = swapped(own, 1)
    first = norms(own, beside, 0)
    slab = summed(picked, 4, 8, devices)
    slab = summed(slab, 4, 2, devices)
    slab = summed(slab, 2, 1, devices)
    beyond = swapped(across, 1)
    second = norms(across, beyond, 2)
    parts = [slab[r * KL : (r + 1) * KL] for r in range(GR)]
    parts = [parts[0]] + [swapped(parts[r], r) for r in range(1, GR)]
    tiles = partial_kernels((own, beside, across, beyond), parts, (first, second), devices, F32)
    tiles = lax.all_to_all(tiles.astype(LINK), "vox", split_axis=0, concat_axis=0, tiled=True)
    tile = jnp.sum(tiles.astype(F32), axis=0)
    turn = [
        (j * devices + z * 8 + x * 2 + y, x * devices + z * 8 + j * 2 + y)
        for j in range(GR)
        for z in range(4)
        for x in range(4)
        for y in range(2)
    ]
    tile = lax.ppermute(tile, ("subj", "vox"), turn)
    return in_order([tile] + [swapped(tile, r) for r in range(1, GR)])


def solution(mesh):
    placed = (P("subj", None, "vox"), P(), P())
    return jax.shard_map(
        body, mesh=mesh, in_specs=placed, out_specs=P("vox", "subj", None), check_vma=False
    )
```

```python
import jax
import jax.numpy as jnp
from jax import lax
from jax.experimental import pallas as pl
from jax.experimental.pallas import tpu as pltpu
from jax.sharding import PartitionSpec as P


TR = 16
EP = 12
GR = 4
SL = 4
SB = GR * SL
KL = 16
VOX = 16384
F32 = jnp.float32
BF16 = jnp.bfloat16
LINK = jnp.float16
series_floor = 1.0
spread_floor = 0.05
shrink_factor = 0.9


def near(x):
    return pltpu.with_memory_space_constraint(x, pltpu.VMEM)


def iota(shape, dim):
    return lax.broadcasted_iota(jnp.int32, shape, dim)


def dot(a, b):
    return jnp.dot(a, b, preferred_element_type=F32)


def dot_nt(a, b):
    return lax.dot_general(a, b, (((1,), (1,)), ((), ())), preferred_element_type=F32)


def split(x):
    hi = x.astype(BF16)
    return hi, (x - hi.astype(F32)).astype(BF16)


def window_kernel(off_ref, sel_ref, series_ref, e_ref, t_ref, w_ref):
    j = lax.axis_index("subj")
    i = lax.axis_index("vox")
    width = series_ref.shape[2]
    lead = iota((TR, series_ref.shape[1]), 1) - iota((TR, series_ref.shape[1]), 0)
    for s in range(SL):
        for e in range(EP):
            chosen = lead == off_ref[j * SL + s, e]
            w_ref[e * TR : (e + 1) * TR, :] = jnp.where(chosen, 1.0, 0.0).astype(BF16)
        rows = dot(w_ref[...], series_ref[s]).astype(BF16)
        for e in range(EP):
            e_ref[e, s * TR : (s + 1) * TR, :] = rows[e * TR : (e + 1) * TR]
    row = iota((GR * KL, 128), 0)
    column = jnp.zeros((GR * KL, 128), jnp.int32)
    for r in range(GR):
        for k in range(KL):
            owner = (k // 4) * 8 + (j ^ r) * 2 + (k // 2) % 2
            column = jnp.where(row == r * KL + k, sel_ref[2 * owner + k % 2] - i * width, column)
    lane = iota((GR * KL, 128), 1)
    picker = jnp.concatenate(
        [jnp.where(column == lane + c, 1.0, 0.0).astype(BF16) for c in range(0, width, 128)], axis=1
    )
    t_ref[...] = dot_nt(picker, e_ref[...].reshape(EP * SL * TR, width)).astype(BF16)


def take_windows(series, offsets, selected):
    width = series.shape[2]
    return pl.pallas_call(
        window_kernel,
        out_shape=(
            pltpu.VMEM((EP, SL * TR, width), BF16),
            pltpu.VMEM((GR * KL, EP * SL * TR), BF16),
        ),
        in_specs=[
            pl.BlockSpec(memory_space=pltpu.SMEM),
            pl.BlockSpec(memory_space=pltpu.SMEM),
            pl.BlockSpec(memory_space=pltpu.VMEM),
        ],
        out_specs=(pl.BlockSpec(memory_space=pltpu.VMEM), pl.BlockSpec(memory_space=pltpu.VMEM)),
        scratch_shapes=[pltpu.VMEM((EP * TR, series.shape[1]), BF16)],
        compiler_params=pltpu.CompilerParams(vmem_limit_bytes=8 << 20),
        name="windows",
    )(
        pltpu.with_memory_space_constraint(offsets, pltpu.HBM),
        pltpu.with_memory_space_constraint(selected, pltpu.HBM),
        pltpu.with_memory_space_constraint(series, pltpu.HBM),
    )


def meeting(j, first, count):
    shape = (SB, count * SL * TR)
    place = iota(shape, 1)
    home = ((place // TR) % SL) * GR + ((place // (SL * TR) + first) ^ j)
    return iota(shape, 0) == home


def norm_kernel(first, e0, e1, n_ref):
    j = lax.axis_index("subj")
    gather = jnp.where(meeting(j, first, 2), 1.0, 0.0).astype(BF16)
    for e in range(EP):
        x = jnp.concatenate([e0[e], e1[e]], axis=0)
        xf = x.astype(F32)
        high, low = split(xf * xf)
        total = dot(gather, x)
        square = dot(gather, high) + dot(gather, low)
        n_ref[e] = square - total * total * (1.0 / TR)


def norms(e0, e1, first):
    return pl.pallas_call(
        lambda *refs: norm_kernel(first, *refs),
        out_shape=pltpu.VMEM((EP, SB, e0.shape[2]), F32),
        in_specs=[pl.BlockSpec(memory_space=pltpu.VMEM)] * 2,
        out_specs=pl.BlockSpec(memory_space=pltpu.VMEM),
        compiler_params=pltpu.CompilerParams(vmem_limit_bytes=4 << 20),
        name="norms",
    )(near(e0), near(e1))


def kernel_kernel(
    e0, e1, e2, e3, s0, s1, s2, s3, na, nb, o_ref, lh_ref, ll_ref, c_ref, z_ref, g_ref
):
    j = lax.axis_index("subj")
    epochs = (e0, e1, e2, e3)
    slabs = (s0, s1, s2, s3)
    width = e0.shape[2]
    deep = SB * TR
    chunk = SL * TR
    same = (iota((deep, deep), 0) // TR == iota((deep, deep), 1) // TR).astype(F32).astype(BF16)
    mine = meeting(j, 0, GR)

    slab = jnp.concatenate(
        [
            jnp.concatenate([s[:, e * chunk : (e + 1) * chunk] for s in slabs], axis=1)
            for e in range(EP)
        ],
        axis=0,
    )
    centred = slab.astype(F32) - dot(slab, same) * (1.0 / TR)
    high, low = split(centred * centred)
    power = dot(high, same) + dot(low, same)
    slab_std = centred * (lax.rsqrt(power + series_floor) * shrink_factor)

    high, low = (half.astype(F32) for half in split(slab_std))
    mine = jnp.where(mine, 1.0, 0.0).astype(BF16)
    for e in range(EP):
        x = jnp.concatenate([p[e] for p in epochs], axis=0)
        norm = jnp.sqrt(na[e] + nb[e] + series_floor)[None]
        for k in range(KL):
            row = slice(e * KL + k, e * KL + k + 1)
            for half, to in ((high, lh_ref), (low, ll_ref)):
                line = jnp.broadcast_to(half[row], mine.shape).astype(BF16) * mine
                to[e % 2, k * SB : (k + 1) * SB, :] = line
        shrunk = dot(lh_ref[e % 2], x) + dot(ll_ref[e % 2], x)
        shrunk = shrunk.reshape(KL, SB, width)
        c_ref[e] = jnp.log((norm + shrunk) / (norm - shrunk)).reshape(KL * SB, width)

    def scores(q, slot):
        for h in range(2):
            rows = pl.ds(pl.multiple_of((q * 2 + h) * SB, SB), SB)
            for c in range(0, width, 128):
                fisher = [c_ref[e, rows, c : c + 128] for e in range(EP)]
                mean = sum(fisher[1:], fisher[0]) * (1.0 / EP)
                fisher = [f - mean for f in fisher]
                spread = fisher[0] * fisher[0]
                for f in fisher[1:]:
                    spread = spread + f * f
                scale = lax.rsqrt(spread * (1.0 / EP) + 4.0 * spread_floor)
                for e in range(EP):
                    at = slice(e * SB, (e + 1) * SB)
                    z_ref[slot, h, at, c : c + 128] = (fisher[e] * scale).astype(BF16)

    def products(q, slot):
        for h in range(2):
            product = dot_nt(z_ref[slot, h], z_ref[slot, h])
            g_ref[slot, h] = product[:, 0:128]
            g_ref[slot, 2, :, h * 64 : (h + 1) * 64] = product[:, 128 : EP * SB]
        for r in range(GR):
            lines = pl.ds(r, EP * SL, stride=GR)
            both = jnp.concatenate([g_ref[slot, n, lines, :] for n in range(3)], axis=0)
            o_ref[(q // 2) * 8 + 2 * r + slot] = both.astype(o_ref.dtype)

    def step(t, carry):
        scores(2 * t + 1, 1)
        products(2 * t, 0)
        scores(2 * t + 2, 0)
        products(2 * t + 1, 1)
        return carry

    last = KL // 2 - 1
    scores(0, 0)
    lax.fori_loop(0, last // 2, step, 0)
    scores(last, 1)
    products(last - 1, 0)
    products(last, 1)


def partial_kernels(epochs, slabs, powers, devices, dtype):
    width = epochs[0].shape[2]
    return pl.pallas_call(
        kernel_kernel,
        out_shape=pltpu.VMEM((devices, 3 * EP * SL, 128), dtype),
        in_specs=[pl.BlockSpec(memory_space=pltpu.VMEM)] * (2 * GR + 2),
        out_specs=pl.BlockSpec(memory_space=pltpu.VMEM),
        scratch_shapes=[
            pltpu.VMEM((2, KL * SB, SB * TR), BF16),
            pltpu.VMEM((2, KL * SB, SB * TR), BF16),
            pltpu.VMEM((EP, KL * SB, width), F32),
            pltpu.VMEM((2, 2, EP * SB, width), BF16),
            pltpu.VMEM((2, 3, EP * SB, 128), F32),
        ],
        compiler_params=pltpu.CompilerParams(vmem_limit_bytes=20 << 20),
        name="partial_kernels",
    )(*map(near, (*epochs, *slabs, *powers)))


def order_kernel(y_ref, o_ref):
    rows = EP * SL
    cols = EP * SB
    source = iota((cols, cols), 0)
    target = (source % GR) * rows + ((source // GR) % SL) * EP + source // SB
    column = jnp.where(iota((cols, cols), 1) == target, 1.0, 0.0).astype(BF16)
    for h in range(2):
        lines = []
        for s in range(SL):
            left = y_ref[pl.ds(h * rows + s, EP, stride=SL), :]
            right = y_ref[pl.ds(2 * rows + s, EP, stride=SL), :]
            lines.append(jnp.concatenate([left, right[:, h * 64 : (h + 1) * 64]], axis=1))
        whole = jnp.concatenate(lines, axis=0)
        high, _ = split(whole)
        middle, low = split(whole - high.astype(F32))
        o_ref[h] = (dot(high, column) + dot(middle, column) + dot(low, column)) * (1.0 / VOX)


def in_order(tile):
    return pl.pallas_call(
        order_kernel,
        out_shape=jax.ShapeDtypeStruct((2, EP * SL, EP * SB), F32),
        in_specs=[pl.BlockSpec(memory_space=pltpu.VMEM)],
        out_specs=pl.BlockSpec(memory_space=pltpu.VMEM),
        compiler_params=pltpu.CompilerParams(vmem_limit_bytes=4 << 20),
        name="in_order",
    )(near(tile))


def ring(step, size, stride, devices):
    def moved(n):
        place = (n // stride) % size
        return n + ((place + step) % size - place) * stride

    return [(n, moved(n)) for n in range(devices)]


def swapped(x, r):
    return lax.ppermute(x, "subj", [(n, n ^ r) for n in range(GR)])


def summed(x, size, stride, devices):
    parts = [lax.ppermute(x, "vox", ring(n, size, stride, devices)) for n in range(1, size)]
    return sum(parts, x)


def body(series, offsets, selected):
    devices = lax.axis_size("vox")
    own, picked = take_windows(series, offsets, selected)
    across = swapped(own, 2)
    beside = swapped(own, 1)
    first = norms(own, beside, 0)
    slab = summed(picked, 4, 8, devices)
    slab = summed(slab, 4, 2, devices)
    slab = summed(slab, 2, 1, devices)
    beyond = swapped(across, 1)
    second = norms(across, beyond, 2)
    parts = [slab[r * KL : (r + 1) * KL] for r in range(GR)]
    parts = [parts[0]] + [swapped(parts[r], r) for r in range(1, GR)]
    tiles = partial_kernels((own, beside, across, beyond), parts, (first, second), devices, F32)
    tiles = lax.all_to_all(tiles.astype(LINK), "vox", split_axis=0, concat_axis=0, tiled=True)
    tile = jnp.sum(tiles.astype(F32), axis=0)
    turn = [
        (j * devices + z * 8 + x * 2 + y, x * devices + z * 8 + j * 2 + y)
        for j in range(GR)
        for z in range(4)
        for x in range(4)
        for y in range(2)
    ]
    return in_order(lax.ppermute(tile, ("subj", "vox"), turn))


def solution(mesh):
    placed = (P("subj", None, "vox"), P(), P())
    return jax.shard_map(
        body, mesh=mesh, in_specs=placed, out_specs=P("vox", "subj", None), check_vma=False
    )
```

```python
import jax
import jax.numpy as jnp
from jax import lax
from jax.experimental import pallas as pl
from jax.experimental.pallas import tpu as pltpu
from jax.sharding import PartitionSpec as P


TR = 16
EP = 12
GR = 4
SL = 4
SB = GR * SL
KL = 16
ROWS = GR * KL
SLOTS = 8
VOX = 16384
F32 = jnp.float32
BF16 = jnp.bfloat16
LINK = jnp.float16
series_floor = 1.0
spread_floor = 0.05
shrink_factor = 0.9


def near(x):
    return pltpu.with_memory_space_constraint(x, pltpu.VMEM)


def far(x):
    return pltpu.with_memory_space_constraint(x, pltpu.HBM)


def iota(shape, dim):
    return lax.broadcasted_iota(jnp.int32, shape, dim)


def dot(a, b):
    return jnp.dot(a, b, preferred_element_type=F32)


def dot_nt(a, b):
    return lax.dot_general(a, b, (((1,), (1,)), ((), ())), preferred_element_type=F32)


def split(x):
    hi = x.astype(BF16)
    return hi, (x - hi.astype(F32)).astype(BF16)


def selected_ids(sel_ref, j):
    row = iota((ROWS, 128), 0)
    lane = iota((8, 128), 1)
    down = jnp.zeros((ROWS, 128), jnp.int32)
    along = jnp.full((8, 128), -VOX, jnp.int32)
    for r in range(GR):
        for k in range(KL):
            voxel = sel_ref[2 * ((k // 4) * 8 + (j ^ r) * 2 + (k // 2) % 2) + k % 2]
            down = jnp.where(row == r * KL + k, voxel, down)
            along = jnp.where(lane == r * KL + k, voxel, along)
    return down, along


def places(down, along, width):
    shift = width.bit_length() - 1
    shard_down = down >> shift
    shard_along = along >> shift
    same = shard_down == jnp.broadcast_to(shard_along[0:1], (ROWS, 128))
    row = iota((ROWS, 128), 0)
    lane = iota((ROWS, 128), 1)
    rank_down = jnp.sum(jnp.where(same & (lane < row), 1.0, 0.0), axis=1, keepdims=True)
    rank_along = jnp.sum(jnp.where(same & (row < lane), 1.0, 0.0), axis=0, keepdims=True)
    return shard_down, rank_down.astype(jnp.int32), shard_along, rank_along.astype(jnp.int32)


def pack_slots(send_ref, picked, shard_along, rank_along, i, turn):
    slot = iota((SLOTS, 128), 0) + turn * SLOTS
    rank = jnp.broadcast_to(rank_along, (SLOTS, 128))
    chosen = (rank == slot) & (shard_along[0:SLOTS] == i)
    chosen = jnp.where(chosen, 1.0, 0.0).astype(BF16)
    slots = dot(chosen[:, 0:ROWS], picked).astype(BF16)
    for n in range(send_ref.shape[0]):
        send_ref[n] = slots


def window_kernel(off_ref, sel_ref, series_ref, e_ref, t_ref, send_ref, turns_ref, w_ref):
    j = lax.axis_index("subj")
    i = lax.axis_index("vox")
    width = series_ref.shape[2]
    lead = iota((TR, series_ref.shape[1]), 1) - iota((TR, series_ref.shape[1]), 0)
    for s in range(SL):
        for e in range(EP):
            chosen = lead == off_ref[j * SL + s, e]
            w_ref[e * TR : (e + 1) * TR, :] = jnp.where(chosen, 1.0, 0.0).astype(BF16)
        rows = dot(w_ref[...], series_ref[s]).astype(BF16)
        for e in range(EP):
            e_ref[e, s * TR : (s + 1) * TR, :] = rows[e * TR : (e + 1) * TR]
    down, along = selected_ids(sel_ref, j)
    lane = iota((ROWS, 128), 1)
    picker = jnp.concatenate(
        [
            jnp.where(down - i * width == lane + c, 1.0, 0.0).astype(BF16)
            for c in range(0, width, 128)
        ],
        axis=1,
    )
    picked = dot_nt(picker, e_ref[...].reshape(EP * SL * TR, width)).astype(BF16)
    t_ref[...] = picked
    _, rank_down, shard_along, rank_along = places(down, along, width)
    pack_slots(send_ref, picked, shard_along, rank_along, i, 0)
    turns_ref[0] = jnp.max(rank_down) // SLOTS + 1


SMEM = pl.BlockSpec(memory_space=pltpu.SMEM)
VMEM = pl.BlockSpec(memory_space=pltpu.VMEM)


def small(mib):
    return pltpu.CompilerParams(vmem_limit_bytes=mib << 20)


def take_windows(series, offsets, selected, devices):
    width = series.shape[2]
    return pl.pallas_call(
        window_kernel,
        out_shape=(
            pltpu.VMEM((EP, SL * TR, width), BF16),
            pltpu.VMEM((ROWS, EP * SL * TR), BF16),
            pltpu.VMEM((devices, SLOTS, EP * SL * TR), BF16),
            jax.ShapeDtypeStruct((1,), jnp.int32),
        ),
        in_specs=[SMEM, SMEM, VMEM],
        out_specs=(VMEM, VMEM, VMEM, SMEM),
        scratch_shapes=[pltpu.VMEM((EP * TR, series.shape[1]), BF16)],
        compiler_params=small(8),
        name="windows",
    )(far(offsets), far(selected), far(series))


def pack_kernel(width, sel_ref, turn_ref, t_ref, send_ref):
    down, along = selected_ids(sel_ref, lax.axis_index("subj"))
    _, _, shard_along, rank_along = places(down, along, width)
    pack_slots(send_ref, t_ref[...], shard_along, rank_along, lax.axis_index("vox"), turn_ref[0])


def pack(selected, turn, picked, devices, width):
    return pl.pallas_call(
        lambda *refs: pack_kernel(width, *refs),
        out_shape=jax.ShapeDtypeStruct((devices, SLOTS, picked.shape[1]), BF16),
        in_specs=[SMEM, SMEM, VMEM],
        out_specs=VMEM,
        compiler_params=small(4),
        name="pack",
    )(selected, turn, picked)


def unpack_kernel(width, sel_ref, turn_ref, r_ref, base_ref, s_ref):
    down, along = selected_ids(sel_ref, lax.axis_index("subj"))
    shard, rank, _, _ = places(down, along, width)
    held = r_ref.shape[0] * SLOTS
    rank = jnp.broadcast_to(rank, (ROWS, 128)) - turn_ref[0] * SLOTS
    source = jnp.where((rank >= 0) & (rank < SLOTS), shard * SLOTS + rank, -1)
    chosen = jnp.concatenate(
        [
            jnp.where(source == iota((ROWS, 128), 1) + c, 1.0, 0.0).astype(BF16)
            for c in range(0, held, 128)
        ],
        axis=1,
    )
    found = dot(chosen, r_ref[...].reshape(held, r_ref.shape[2]))
    s_ref[...] = (base_ref[...].astype(F32) + found).astype(BF16)


def unpack(selected, turn, arrived, base, width):
    return pl.pallas_call(
        lambda *refs: unpack_kernel(width, *refs),
        out_shape=jax.ShapeDtypeStruct(base.shape, BF16),
        in_specs=[SMEM, SMEM, VMEM, VMEM],
        out_specs=VMEM,
        compiler_params=small(4),
        name="unpack",
    )(selected, turn, arrived, base)


def meeting(j, first, count):
    shape = (SB, count * SL * TR)
    place = iota(shape, 1)
    home = ((place // TR) % SL) * GR + ((place // (SL * TR) + first) ^ j)
    return iota(shape, 0) == home


def norm_kernel(first, e0, e1, n_ref):
    j = lax.axis_index("subj")
    gather = jnp.where(meeting(j, first, 2), 1.0, 0.0).astype(BF16)
    for e in range(EP):
        x = jnp.concatenate([e0[e], e1[e]], axis=0)
        xf = x.astype(F32)
        high, low = split(xf * xf)
        total = dot(gather, x)
        square = dot(gather, high) + dot(gather, low)
        n_ref[e] = square - total * total * (1.0 / TR)


def norms(e0, e1, first):
    return pl.pallas_call(
        lambda *refs: norm_kernel(first, *refs),
        out_shape=pltpu.VMEM((EP, SB, e0.shape[2]), F32),
        in_specs=[pl.BlockSpec(memory_space=pltpu.VMEM)] * 2,
        out_specs=pl.BlockSpec(memory_space=pltpu.VMEM),
        compiler_params=pltpu.CompilerParams(vmem_limit_bytes=4 << 20),
        name="norms",
    )(near(e0), near(e1))


def kernel_kernel(
    e0, e1, e2, e3, s0, s1, s2, s3, na, nb, o_ref, lh_ref, ll_ref, c_ref, z_ref, g_ref
):
    j = lax.axis_index("subj")
    epochs = (e0, e1, e2, e3)
    slabs = (s0, s1, s2, s3)
    width = e0.shape[2]
    deep = SB * TR
    chunk = SL * TR
    same = (iota((deep, deep), 0) // TR == iota((deep, deep), 1) // TR).astype(F32).astype(BF16)
    mine = meeting(j, 0, GR)

    slab = jnp.concatenate(
        [
            jnp.concatenate([s[:, e * chunk : (e + 1) * chunk] for s in slabs], axis=1)
            for e in range(EP)
        ],
        axis=0,
    )
    centred = slab.astype(F32) - dot(slab, same) * (1.0 / TR)
    high, low = split(centred * centred)
    power = dot(high, same) + dot(low, same)
    slab_std = centred * (lax.rsqrt(power + series_floor) * shrink_factor)

    high, low = (half.astype(F32) for half in split(slab_std))
    mine = jnp.where(mine, 1.0, 0.0).astype(BF16)
    for e in range(EP):
        x = jnp.concatenate([p[e] for p in epochs], axis=0)
        norm = jnp.sqrt(na[e] + nb[e] + series_floor)[None]
        for k in range(KL):
            row = slice(e * KL + k, e * KL + k + 1)
            for half, to in ((high, lh_ref), (low, ll_ref)):
                line = jnp.broadcast_to(half[row], mine.shape).astype(BF16) * mine
                to[e % 2, k * SB : (k + 1) * SB, :] = line
        shrunk = dot(lh_ref[e % 2], x) + dot(ll_ref[e % 2], x)
        shrunk = shrunk.reshape(KL, SB, width)
        c_ref[e] = jnp.log((norm + shrunk) / (norm - shrunk)).reshape(KL * SB, width)

    def scores(q, slot):
        for h in range(2):
            rows = pl.ds(pl.multiple_of((q * 2 + h) * SB, SB), SB)
            for c in range(0, width, 128):
                fisher = [c_ref[e, rows, c : c + 128] for e in range(EP)]
                mean = sum(fisher[1:], fisher[0]) * (1.0 / EP)
                fisher = [f - mean for f in fisher]
                spread = fisher[0] * fisher[0]
                for f in fisher[1:]:
                    spread = spread + f * f
                scale = lax.rsqrt(spread * (1.0 / EP) + 4.0 * spread_floor)
                for e in range(EP):
                    at = slice(e * SB, (e + 1) * SB)
                    z_ref[slot, h, at, c : c + 128] = (fisher[e] * scale).astype(BF16)

    def products(q, slot):
        for h in range(2):
            product = dot_nt(z_ref[slot, h], z_ref[slot, h])
            g_ref[slot, h] = product[:, 0:128]
            g_ref[slot, 2, :, h * 64 : (h + 1) * 64] = product[:, 128 : EP * SB]
        for r in range(GR):
            lines = pl.ds(r, EP * SL, stride=GR)
            both = jnp.concatenate([g_ref[slot, n, lines, :] for n in range(3)], axis=0)
            o_ref[(q // 2) * 8 + 2 * r + slot] = both.astype(o_ref.dtype)

    def step(t, carry):
        scores(2 * t + 1, 1)
        products(2 * t, 0)
        scores(2 * t + 2, 0)
        products(2 * t + 1, 1)
        return carry

    last = KL // 2 - 1
    scores(0, 0)
    lax.fori_loop(0, last // 2, step, 0)
    scores(last, 1)
    products(last - 1, 0)
    products(last, 1)


def partial_kernels(epochs, slabs, powers, devices, dtype):
    width = epochs[0].shape[2]
    return pl.pallas_call(
        kernel_kernel,
        out_shape=pltpu.VMEM((devices, 3 * EP * SL, 128), dtype),
        in_specs=[pl.BlockSpec(memory_space=pltpu.VMEM)] * (2 * GR + 2),
        out_specs=pl.BlockSpec(memory_space=pltpu.VMEM),
        scratch_shapes=[
            pltpu.VMEM((2, KL * SB, SB * TR), BF16),
            pltpu.VMEM((2, KL * SB, SB * TR), BF16),
            pltpu.VMEM((EP, KL * SB, width), F32),
            pltpu.VMEM((2, 2, EP * SB, width), BF16),
            pltpu.VMEM((2, 3, EP * SB, 128), F32),
        ],
        compiler_params=pltpu.CompilerParams(vmem_limit_bytes=20 << 20),
        name="partial_kernels",
    )(*map(near, (*epochs, *slabs, *powers)))


def order_kernel(y_ref, o_ref):
    rows = EP * SL
    cols = EP * SB
    source = iota((cols, cols), 0)
    target = (source % GR) * rows + ((source // GR) % SL) * EP + source // SB
    column = jnp.where(iota((cols, cols), 1) == target, 1.0, 0.0).astype(BF16)
    for h in range(2):
        lines = []
        for s in range(SL):
            left = y_ref[pl.ds(h * rows + s, EP, stride=SL), :]
            right = y_ref[pl.ds(2 * rows + s, EP, stride=SL), :]
            lines.append(jnp.concatenate([left, right[:, h * 64 : (h + 1) * 64]], axis=1))
        whole = jnp.concatenate(lines, axis=0)
        high, _ = split(whole)
        middle, low = split(whole - high.astype(F32))
        o_ref[h] = (dot(high, column) + dot(middle, column) + dot(low, column)) * (1.0 / VOX)


def in_order(tile):
    return pl.pallas_call(
        order_kernel,
        out_shape=jax.ShapeDtypeStruct((2, EP * SL, EP * SB), F32),
        in_specs=[pl.BlockSpec(memory_space=pltpu.VMEM)],
        out_specs=pl.BlockSpec(memory_space=pltpu.VMEM),
        compiler_params=pltpu.CompilerParams(vmem_limit_bytes=4 << 20),
        name="in_order",
    )(near(tile))


def swapped(x, r):
    return lax.ppermute(x, "subj", [(n, n ^ r) for n in range(GR)])


def whole_slab(selected, picked, send, turns, devices, width):
    def exchanged(send, turn, base):
        arrived = lax.all_to_all(send, "vox", split_axis=0, concat_axis=0, tiled=True)
        return unpack(selected, turn, arrived, base, width)

    def again(state):
        turn, slab = state
        send = pack(selected, turn, picked, devices, width)
        return turn + 1, exchanged(send, turn, slab)

    slab = exchanged(send, jnp.zeros((1,), jnp.int32), jnp.zeros_like(picked))
    first = jnp.ones((1,), jnp.int32)
    return lax.while_loop(lambda state: state[0][0] < turns[0], again, (first, slab))[1]


def body(series, offsets, selected):
    devices = lax.axis_size("vox")
    own, picked, send, turns = take_windows(series, offsets, selected, devices)
    across = swapped(own, 2)
    beside = swapped(own, 1)
    first = norms(own, beside, 0)
    slab = whole_slab(selected, picked, send, turns, devices, series.shape[2])
    beyond = swapped(across, 1)
    second = norms(across, beyond, 2)
    parts = [slab[r * KL : (r + 1) * KL] for r in range(GR)]
    parts = [parts[0]] + [swapped(parts[r], r) for r in range(1, GR)]
    tiles = partial_kernels(
        (own, beside, across, beyond), parts, (first, second), devices, F32
    )
    tiles = lax.all_to_all(tiles.astype(LINK), "vox", split_axis=0, concat_axis=0, tiled=True)
    tile = jnp.sum(tiles.astype(F32), axis=0)
    turn = [
        (j * devices + z * 8 + x * 2 + y, x * devices + z * 8 + j * 2 + y)
        for j in range(GR)
        for z in range(4)
        for x in range(4)
        for y in range(2)
    ]
    return in_order(lax.ppermute(tile, ("subj", "vox"), turn))


def solution(mesh):
    placed = (P("subj", None, "vox"), P(), P())
    return jax.shard_map(
        body, mesh=mesh, in_specs=placed, out_specs=P("vox", "subj", None), check_vma=False
    )
```

```python
import jax
import jax.numpy as jnp
from jax import lax
from jax.experimental import pallas as pl
from jax.experimental.pallas import tpu as pltpu
from jax.sharding import PartitionSpec as P


TR = 16
EP = 12
GR = 4
SL = 4
SB = GR * SL
KL = 16
VOX = 16384
F32 = jnp.float32
BF16 = jnp.bfloat16
LINK = jnp.float16
series_floor = 1.0
spread_floor = 0.05
shrink_factor = 0.9


def near(x):
    return pltpu.with_memory_space_constraint(x, pltpu.VMEM)


def iota(shape, dim):
    return lax.broadcasted_iota(jnp.int32, shape, dim)


def dot(a, b):
    return jnp.dot(a, b, preferred_element_type=F32)


def dot_nt(a, b):
    return lax.dot_general(a, b, (((1,), (1,)), ((), ())), preferred_element_type=F32)


def split(x):
    hi = x.astype(BF16)
    return hi, (x - hi.astype(F32)).astype(BF16)


def owner(g, p):
    return (p // 2) * 8 + ((p % 2) * 2 + g % 2) * 2 + g // 2


def window_kernel(off_ref, sel_ref, series_ref, e_ref, keep_ref, give_ref, w_ref):
    j = lax.axis_index("subj")
    i = lax.axis_index("vox")
    width = series_ref.shape[2]
    lead = iota((TR, series_ref.shape[1]), 1) - iota((TR, series_ref.shape[1]), 0)
    for s in range(SL):
        for e in range(EP):
            chosen = lead == off_ref[j * SL + s, e]
            w_ref[e * TR : (e + 1) * TR, :] = jnp.where(chosen, 1.0, 0.0).astype(BF16)
        rows = dot(w_ref[...], series_ref[s]).astype(BF16)
        for e in range(EP):
            e_ref[e, s * TR : (s + 1) * TR, :] = rows[e * TR : (e + 1) * TR]
    row = iota((GR * KL, 128), 0)
    column = jnp.zeros((GR * KL, 128), jnp.int32)
    for b, r in enumerate((0, 2, 1, 3)):
        for k in range(KL):
            voxel = sel_ref[2 * owner(j ^ r, k // 2) + k % 2]
            column = jnp.where(row == b * KL + k, voxel - i * width, column)
    lane = iota((GR * KL, 128), 1)
    picker = jnp.concatenate(
        [jnp.where(column == lane + c, 1.0, 0.0).astype(BF16) for c in range(0, width, 128)], axis=1
    )
    picked = dot_nt(picker, e_ref[...].reshape(EP * SL * TR, width)).astype(BF16)
    keep_ref[...] = picked[0 : 2 * KL]
    give_ref[...] = picked[2 * KL :]


def take_windows(series, offsets, selected):
    width = series.shape[2]
    return pl.pallas_call(
        window_kernel,
        out_shape=(
            pltpu.VMEM((EP, SL * TR, width), BF16),
            pltpu.VMEM((2 * KL, EP * SL * TR), BF16),
            pltpu.VMEM((2 * KL, EP * SL * TR), BF16),
        ),
        in_specs=[
            pl.BlockSpec(memory_space=pltpu.SMEM),
            pl.BlockSpec(memory_space=pltpu.SMEM),
            pl.BlockSpec(memory_space=pltpu.VMEM),
        ],
        out_specs=(pl.BlockSpec(memory_space=pltpu.VMEM),) * 3,
        scratch_shapes=[pltpu.VMEM((EP * TR, series.shape[1]), BF16)],
        compiler_params=pltpu.CompilerParams(vmem_limit_bytes=8 << 20),
        name="windows",
    )(
        pltpu.with_memory_space_constraint(offsets, pltpu.HBM),
        pltpu.with_memory_space_constraint(selected, pltpu.HBM),
        pltpu.with_memory_space_constraint(series, pltpu.HBM),
    )


def meeting(j, first, count):
    shape = (SB, count * SL * TR)
    place = iota(shape, 1)
    home = ((place // TR) % SL) * GR + ((place // (SL * TR) + first) ^ j)
    return iota(shape, 0) == home


def norm_kernel(first, e0, e1, n_ref):
    j = lax.axis_index("subj")
    gather = jnp.where(meeting(j, first, 2), 1.0, 0.0).astype(BF16)
    for e in range(EP):
        x = jnp.concatenate([e0[e], e1[e]], axis=0)
        xf = x.astype(F32)
        high, low = split(xf * xf)
        total = dot(gather, x)
        square = dot(gather, high) + dot(gather, low)
        n_ref[e] = square - total * total * (1.0 / TR)


def norms(e0, e1, first):
    return pl.pallas_call(
        lambda *refs: norm_kernel(first, *refs),
        out_shape=pltpu.VMEM((EP, SB, e0.shape[2]), F32),
        in_specs=[pl.BlockSpec(memory_space=pltpu.VMEM)] * 2,
        out_specs=pl.BlockSpec(memory_space=pltpu.VMEM),
        compiler_params=pltpu.CompilerParams(vmem_limit_bytes=4 << 20),
        name="norms",
    )(near(e0), near(e1))


def kernel_kernel(
    e0, e1, e2, e3, s0, s1, s2, s3, na, nb, o_ref, lh_ref, ll_ref, c_ref, z_ref, g_ref
):
    j = lax.axis_index("subj")
    epochs = (e0, e1, e2, e3)
    slabs = []
    for one, other in ((s0, s1), (s2, s3)):
        both = (one[...].astype(F32) + other[...].astype(F32)).astype(BF16)
        slabs += [both[0:KL], both[KL : 2 * KL]]
    width = e0.shape[2]
    deep = SB * TR
    chunk = SL * TR
    same = (iota((deep, deep), 0) // TR == iota((deep, deep), 1) // TR).astype(F32).astype(BF16)
    mine = meeting(j, 0, GR)

    slab = jnp.concatenate(
        [
            jnp.concatenate([s[:, e * chunk : (e + 1) * chunk] for s in slabs], axis=1)
            for e in range(EP)
        ],
        axis=0,
    )
    centred = slab.astype(F32) - dot(slab, same) * (1.0 / TR)
    high, low = split(centred * centred)
    power = dot(high, same) + dot(low, same)
    slab_std = centred * (lax.rsqrt(power + series_floor) * shrink_factor)

    high, low = (half.astype(F32) for half in split(slab_std))
    mine = jnp.where(mine, 1.0, 0.0).astype(BF16)
    for e in range(EP):
        x = jnp.concatenate([p[e] for p in epochs], axis=0)
        norm = jnp.sqrt(na[e] + nb[e] + series_floor)[None]
        for k in range(KL):
            row = slice(e * KL + k, e * KL + k + 1)
            for half, to in ((high, lh_ref), (low, ll_ref)):
                line = jnp.broadcast_to(half[row], mine.shape).astype(BF16) * mine
                to[e % 2, k * SB : (k + 1) * SB, :] = line
        shrunk = dot(lh_ref[e % 2], x) + dot(ll_ref[e % 2], x)
        shrunk = shrunk.reshape(KL, SB, width)
        c_ref[e] = jnp.log((norm + shrunk) / (norm - shrunk)).reshape(KL * SB, width)

    def scores(q, slot):
        for h in range(2):
            rows = pl.ds(pl.multiple_of((q * 2 + h) * SB, SB), SB)
            for c in range(0, width, 128):
                fisher = [c_ref[e, rows, c : c + 128] for e in range(EP)]
                mean = sum(fisher[1:], fisher[0]) * (1.0 / EP)
                fisher = [f - mean for f in fisher]
                spread = fisher[0] * fisher[0]
                for f in fisher[1:]:
                    spread = spread + f * f
                scale = lax.rsqrt(spread * (1.0 / EP) + 4.0 * spread_floor)
                for e in range(EP):
                    at = slice(e * SB, (e + 1) * SB)
                    z_ref[slot, h, at, c : c + 128] = (fisher[e] * scale).astype(BF16)

    def products(q, slot):
        for h in range(2):
            product = dot_nt(z_ref[slot, h], z_ref[slot, h])
            g_ref[slot, h] = product[:, 0:128]
            g_ref[slot, 2, :, h * 64 : (h + 1) * 64] = product[:, 128 : EP * SB]
        for r in range(GR):
            lines = pl.ds(r, EP * SL, stride=GR)
            both = jnp.concatenate([g_ref[slot, n, lines, :] for n in range(3)], axis=0)
            o_ref[(q // 2) * 8 + slot * 4 + (r % 2) * 2 + r // 2] = both.astype(o_ref.dtype)

    def step(t, carry):
        scores(2 * t + 1, 1)
        products(2 * t, 0)
        scores(2 * t + 2, 0)
        products(2 * t + 1, 1)
        return carry

    last = KL // 2 - 1
    scores(0, 0)
    lax.fori_loop(0, last // 2, step, 0)
    scores(last, 1)
    products(last - 1, 0)
    products(last, 1)


def partial_kernels(epochs, slabs, powers, devices, dtype):
    width = epochs[0].shape[2]
    return pl.pallas_call(
        kernel_kernel,
        out_shape=pltpu.VMEM((devices, 3 * EP * SL, 128), dtype),
        in_specs=[pl.BlockSpec(memory_space=pltpu.VMEM)] * (2 * GR + 2),
        out_specs=pl.BlockSpec(memory_space=pltpu.VMEM),
        scratch_shapes=[
            pltpu.VMEM((2, KL * SB, SB * TR), BF16),
            pltpu.VMEM((2, KL * SB, SB * TR), BF16),
            pltpu.VMEM((EP, KL * SB, width), F32),
            pltpu.VMEM((2, 2, EP * SB, width), BF16),
            pltpu.VMEM((2, 3, EP * SB, 128), F32),
        ],
        compiler_params=pltpu.CompilerParams(vmem_limit_bytes=20 << 20),
        name="partial_kernels",
    )(*map(near, (*epochs, *slabs, *powers)))


def order_kernel(y_ref, o_ref):
    rows = EP * SL
    cols = EP * SB
    source = iota((cols, cols), 0)
    target = (source % GR) * rows + ((source // GR) % SL) * EP + source // SB
    column = jnp.where(iota((cols, cols), 1) == target, 1.0, 0.0).astype(BF16)
    for h in range(2):
        lines = []
        for s in range(SL):
            left = y_ref[pl.ds(h * rows + s, EP, stride=SL), :]
            right = y_ref[pl.ds(2 * rows + s, EP, stride=SL), :]
            lines.append(jnp.concatenate([left, right[:, h * 64 : (h + 1) * 64]], axis=1))
        whole = jnp.concatenate(lines, axis=0)
        high, _ = split(whole)
        middle, low = split(whole - high.astype(F32))
        o_ref[h] = (dot(high, column) + dot(middle, column) + dot(low, column)) * (1.0 / VOX)


def in_order(tile):
    return pl.pallas_call(
        order_kernel,
        out_shape=jax.ShapeDtypeStruct((2, EP * SL, EP * SB), F32),
        in_specs=[pl.BlockSpec(memory_space=pltpu.VMEM)],
        out_specs=pl.BlockSpec(memory_space=pltpu.VMEM),
        compiler_params=pltpu.CompilerParams(vmem_limit_bytes=4 << 20),
        name="in_order",
    )(near(tile))


def ring(step, size, stride, devices):
    def moved(n):
        place = (n // stride) % size
        return n + ((place + step) % size - place) * stride

    return [(n, moved(n)) for n in range(devices)]


def swapped(x, r):
    return lax.ppermute(x, "subj", [(n, n ^ r) for n in range(GR)])


def summed(x, size, stride, devices):
    parts = [lax.ppermute(x, "vox", ring(n, size, stride, devices)) for n in range(1, size)]
    return sum(parts, x)


def along_y(x, chips, halves, devices):
    moves = [
        (j * devices + i, (j ^ (2 * chips)) * devices + (i ^ halves))
        for j in range(GR)
        for i in range(devices)
    ]
    return lax.ppermute(x, ("subj", "vox"), moves)


def body(series, offsets, selected):
    devices = lax.axis_size("vox")
    own, keep, give = take_windows(series, offsets, selected)
    taken = swapped(give, 1)
    across = swapped(own, 2)
    beside = swapped(own, 1)
    first = norms(own, beside, 0)
    slab = jnp.concatenate([keep[:KL], taken[:KL], keep[KL:], taken[KL:]], axis=0)
    slab = summed(slab, 4, 8, devices)
    slab = summed(slab, 4, 2, devices)
    beyond = swapped(across, 1)
    mine, theirs = slab[: 2 * KL], slab[2 * KL :]
    parts = [
        mine,
        along_y(mine, 0, 1, devices),
        along_y(theirs, 1, 0, devices),
        along_y(theirs, 1, 1, devices),
    ]
    second = norms(across, beyond, 2)
    tiles = partial_kernels(
        (own, beside, across, beyond), parts, (first, second), devices, F32
    )
    tiles = lax.all_to_all(tiles.astype(LINK), "vox", split_axis=0, concat_axis=0, tiled=True)
    tile = jnp.sum(tiles.astype(F32), axis=0)
    turn = [
        (
            j * devices + z * 8 + x * 2 + y,
            (2 * y + x % 2) * devices + z * 8 + (x // 2 * 2 + j % 2) * 2 + j // 2,
        )
        for j in range(GR)
        for z in range(4)
        for x in range(4)
        for y in range(2)
    ]
    return in_order(lax.ppermute(tile, ("subj", "vox"), turn))


def solution(mesh):
    placed = (P("subj", None, "vox"), P(), P())
    return jax.shard_map(
        body, mesh=mesh, in_specs=placed, out_specs=P("vox", "subj", None), check_vma=False
    )
```

```python
import jax
import jax.numpy as jnp
from jax import lax
from jax.experimental import pallas as pl
from jax.experimental.pallas import tpu as pltpu
from jax.sharding import PartitionSpec as P


TR = 16
EP = 12
GR = 4
SL = 4
SB = GR * SL
KL = 16
PART = 2 * SL
HALF = EP * SB // 3
BLOCKS = ((0, 0), (0, 1), (0, 2), (1, 1), (1, 2), (2, 2))
QUARTER = len(BLOCKS) * HALF // GR
VOX = 16384
F32 = jnp.float32
BF16 = jnp.bfloat16
LINK = jnp.float16
series_floor = 1.0
spread_floor = 0.05
shrink_factor = 0.9


def near(x):
    return pltpu.with_memory_space_constraint(x, pltpu.VMEM)


SMEM = pl.BlockSpec(memory_space=pltpu.SMEM)
VMEM = pl.BlockSpec(memory_space=pltpu.VMEM)


def small(mib):
    return pltpu.CompilerParams(vmem_limit_bytes=mib << 20)


def iota(shape, dim):
    return lax.broadcasted_iota(jnp.int32, shape, dim)


def dot(a, b):
    return jnp.dot(a, b, preferred_element_type=F32)


def dot_nt(a, b):
    return lax.dot_general(a, b, (((1,), (1,)), ((), ())), preferred_element_type=F32)


def split(x):
    hi = x.astype(BF16)
    return hi, (x - hi.astype(F32)).astype(BF16)


def owner(g, p):
    return (p // 2) * 8 + ((p % 2) * 2 + g % 2) * 2 + g // 2


def window_kernel(off_ref, sel_ref, series_ref, e_ref, keep_ref, give_ref, w_ref):
    j = lax.axis_index("subj")
    i = lax.axis_index("vox")
    width = series_ref.shape[2]
    lead = iota((TR, series_ref.shape[1]), 1) - iota((TR, series_ref.shape[1]), 0)
    for s in range(SL):
        for e in range(EP):
            chosen = lead == off_ref[j * SL + s, e]
            w_ref[e * TR : (e + 1) * TR, :] = jnp.where(chosen, 1.0, 0.0).astype(BF16)
        rows = dot(w_ref[...], series_ref[s]).astype(BF16)
        for e in range(EP):
            e_ref[e, s * TR : (s + 1) * TR, :] = rows[e * TR : (e + 1) * TR]
    row = iota((GR * KL, 128), 0)
    column = jnp.zeros((GR * KL, 128), jnp.int32)
    for b, r in enumerate((0, 2, 1, 3)):
        for k in range(KL):
            voxel = sel_ref[2 * owner(j ^ r, k // 2) + k % 2]
            column = jnp.where(row == b * KL + k, voxel - i * width, column)
    lane = iota((GR * KL, 128), 1)
    picker = jnp.concatenate(
        [jnp.where(column == lane + c, 1.0, 0.0).astype(BF16) for c in range(0, width, 128)], axis=1
    )
    picked = dot_nt(picker, e_ref[...].reshape(EP * SL * TR, width)).astype(BF16)
    keep_ref[...] = picked[0 : 2 * KL]
    give_ref[...] = picked[2 * KL :]


def take_windows(series, offsets, selected):
    width = series.shape[2]
    return pl.pallas_call(
        window_kernel,
        out_shape=(
            pltpu.VMEM((EP, SL * TR, width), BF16),
            pltpu.VMEM((2 * KL, EP * SL * TR), BF16),
            pltpu.VMEM((2 * KL, EP * SL * TR), BF16),
        ),
        in_specs=[
            pl.BlockSpec(memory_space=pltpu.SMEM),
            pl.BlockSpec(memory_space=pltpu.SMEM),
            pl.BlockSpec(memory_space=pltpu.VMEM),
        ],
        out_specs=(pl.BlockSpec(memory_space=pltpu.VMEM),) * 3,
        scratch_shapes=[pltpu.VMEM((EP * TR, series.shape[1]), BF16)],
        compiler_params=pltpu.CompilerParams(vmem_limit_bytes=8 << 20),
        name="windows",
    )(
        pltpu.with_memory_space_constraint(offsets, pltpu.HBM),
        pltpu.with_memory_space_constraint(selected, pltpu.HBM),
        pltpu.with_memory_space_constraint(series, pltpu.HBM),
    )


def meeting(j):
    place = iota((PART, 2 * SL * TR), 1)
    home = ((place // TR) % SL) * 2 + ((place // (SL * TR)) ^ j) % 2
    return iota((PART, 2 * SL * TR), 0) == home


def norm_kernel(e0, e1, n_ref):
    gather = jnp.where(meeting(lax.axis_index("subj")), 1.0, 0.0).astype(BF16)
    for e in range(EP):
        x = jnp.concatenate([e0[e], e1[e]], axis=0)
        xf = x.astype(F32)
        high, low = split(xf * xf)
        total = dot(gather, x)
        square = dot(gather, high) + dot(gather, low)
        n_ref[e] = square - total * total * (1.0 / TR)


def norms(e0, e1):
    return pl.pallas_call(
        norm_kernel,
        out_shape=pltpu.VMEM((EP, PART, e0.shape[2]), F32),
        in_specs=[VMEM] * 2,
        out_specs=VMEM,
        compiler_params=small(4),
        name="norms",
    )(near(e0), near(e1))


def fisher_kernel(e0, e1, s0, s1, n_ref, f_ref, l_ref):
    width = e0.shape[2]
    deep = 2 * SL * TR
    chunk = SL * TR
    mine = jnp.where(meeting(lax.axis_index("subj")), 1.0, 0.0)
    mine = jnp.concatenate([mine, mine], axis=0).astype(BF16)
    same = (iota((deep, deep), 0) // TR == iota((deep, deep), 1) // TR).astype(F32).astype(BF16)
    both = (s0[...].astype(F32) + s1[...].astype(F32)).astype(BF16)
    slab = jnp.concatenate(
        [
            jnp.concatenate([both[r : r + KL, e * chunk : (e + 1) * chunk] for r in (0, KL)], axis=1)
            for e in range(EP)
        ],
        axis=0,
    )
    centred = slab.astype(F32) - dot(slab, same) * (1.0 / TR)
    high, low = split(centred * centred)
    power = dot(high, same) + dot(low, same)
    slab_std = centred * (lax.rsqrt(power + series_floor) * shrink_factor)
    halves = [half.astype(F32) for half in split(slab_std)]
    for e in range(EP):
        x = jnp.concatenate([e0[e], e1[e]] * 2, axis=0)
        norm = jnp.sqrt(n_ref[e] + series_floor)[None]
        for k in range(0, KL, 2):
            for n, half in enumerate(halves):
                row = e * KL + k
                line = [jnp.broadcast_to(half[r : r + 1], (PART, deep)) for r in (row, row + 1)]
                line = jnp.concatenate(line, axis=0).astype(BF16) * mine
                l_ref[e % 2, k * PART : (k + 2) * PART, n * deep : (n + 1) * deep] = line
        shrunk = dot(l_ref[e % 2], x).reshape(KL, PART, width)
        f_ref[e] = jnp.log((norm + shrunk) / (norm - shrunk)).reshape(KL * PART, width)


def fishers(e0, e1, s0, s1, power):
    width = e0.shape[2]
    return pl.pallas_call(
        fisher_kernel,
        out_shape=pltpu.VMEM((EP, KL * PART, width), F32),
        in_specs=[VMEM] * 5,
        out_specs=VMEM,
        scratch_shapes=[pltpu.VMEM((2, KL * PART, 4 * SL * TR), BF16)],
        compiler_params=small(8),
        name="fishers",
    )(*map(near, (e0, e1, s0, s1, power)))


def kernel_kernel(fa, fb, o_ref, z_ref):
    width = fa.shape[2]

    def scores(q, slot):
        for h in range(2):
            rows = pl.ds(pl.multiple_of((q * 2 + h) * PART, PART), PART)
            for c in range(0, width, 128):
                tiles = []
                for f_ref in (fa, fb):
                    fisher = [f_ref[e, rows, c : c + 128] for e in range(EP)]
                    mean = sum(fisher[1:], fisher[0]) * (1.0 / EP)
                    fisher = [f - mean for f in fisher]
                    spread = fisher[0] * fisher[0]
                    for f in fisher[1:]:
                        spread = spread + f * f
                    scale = lax.rsqrt(spread * (1.0 / EP) + 4.0 * spread_floor)
                    tiles.append([f * scale for f in fisher])
                for e in range(EP):
                    tile = jnp.concatenate([tiles[0][e], tiles[1][e]], axis=0).astype(BF16)
                    z_ref[slot, h, e * SB : (e + 1) * SB, c : c + 128] = tile

    def products(q, slot):
        for h in range(2):
            product = dot_nt(z_ref[slot, h], z_ref[slot, h])
            for n, (low, high) in enumerate(BLOCKS):
                tile = product[low * HALF : (low + 1) * HALF, high * HALF : (high + 1) * HALF]
                for first in range(0, HALF, HALF // 2):
                    r, line = divmod(n * HALF + first, QUARTER)
                    to = (q // 2) * 8 + (slot * 2 + r % 2) * 2 + r // 2
                    part = tile[first : first + HALF // 2]
                    o_ref[to, line : line + HALF // 2, h * HALF : (h + 1) * HALF] = part

    def step(t, carry):
        scores(2 * t + 1, 1)
        products(2 * t, 0)
        scores(2 * t + 2, 0)
        products(2 * t + 1, 1)
        return carry

    last = KL // 2 - 1
    scores(0, 0)
    lax.fori_loop(0, last // 2, step, 0)
    scores(last, 1)
    products(last - 1, 0)
    products(last, 1)


def partial_kernels(fa, fb, devices):
    width = fa.shape[2]
    return pl.pallas_call(
        kernel_kernel,
        out_shape=pltpu.VMEM((devices, QUARTER, 2 * HALF), F32),
        in_specs=[VMEM] * 2,
        out_specs=VMEM,
        scratch_shapes=[pltpu.VMEM((2, 2, EP * SB, width), BF16)],
        compiler_params=small(8),
        name="partial_kernels",
    )(near(fa), near(fb))


def order_kernel(y0, y1, y2, y3, o_ref, b_ref, k_ref):
    j = lax.axis_index("subj")
    for r, y in enumerate((y0, y1, y2, y3)):
        b_ref[pl.ds(pl.multiple_of((j ^ r) * QUARTER, QUARTER), QUARTER), :] = y[...]
    for n, (low, high) in enumerate(BLOCKS):
        tile = b_ref[n * HALF : (n + 1) * HALF, :]
        mirrored = tile.T
        for h in range(2):
            block = tile[:, h * HALF : (h + 1) * HALF]
            at = (high % 2) * HALF
            k_ref[h, high // 2, low * HALF : (low + 1) * HALF, at : at + HALF] = block
            if low != high:
                block = mirrored[h * HALF : (h + 1) * HALF]
                at = (low % 2) * HALF
                k_ref[h, low // 2, high * HALF : (high + 1) * HALF, at : at + HALF] = block
    cols = EP * SB
    turn = lax.axis_index("vox") % 2
    source = iota((cols, cols), 0)
    group = (((source // PART) % 2) ^ turn) * 2 + source % 2
    target = group * (EP * SL) + ((source // 2) % SL) * EP + source // SB
    column = jnp.where(iota((cols, cols), 1) == target, 1.0, 0.0).astype(BF16)
    for h in range(2):
        lines = []
        for s in range(SL):
            own = pl.ds((j // 2 ^ turn) * PART + s * 2 + j % 2, EP, stride=SB)
            lines.append(jnp.concatenate([k_ref[h, 0, own, :], k_ref[h, 1, own, :][:, 0:HALF]], axis=1))
        whole = jnp.concatenate(lines, axis=0)
        high, _ = split(whole)
        middle, low = split(whole - high.astype(F32))
        o_ref[h] = (dot(high, column) + dot(middle, column) + dot(low, column)) * (1.0 / VOX)


def in_order(tiles):
    return pl.pallas_call(
        order_kernel,
        out_shape=jax.ShapeDtypeStruct((2, EP * SL, EP * SB), F32),
        in_specs=[pl.BlockSpec(memory_space=pltpu.VMEM)] * GR,
        out_specs=pl.BlockSpec(memory_space=pltpu.VMEM),
        scratch_shapes=[
            pltpu.VMEM((len(BLOCKS) * HALF, 2 * HALF), F32),
            pltpu.VMEM((2, 2, EP * SB, 2 * HALF), F32),
        ],
        compiler_params=pltpu.CompilerParams(vmem_limit_bytes=4 << 20),
        name="in_order",
    )(*map(near, tiles))


def swapped(x, r):
    return lax.ppermute(x, "subj", [(n, n ^ r) for n in range(GR)])


def summed(x, stride, devices):
    parts = [
        lax.ppermute(x, "vox", [(n, n ^ (step * stride)) for n in range(devices)])
        for step in (1, 3, 2)
    ]
    return sum(parts, x)


def along_y(x, chips, halves, devices):
    moves = [
        (j * devices + i, (j ^ (2 * chips)) * devices + (i ^ halves))
        for j in range(GR)
        for i in range(devices)
    ]
    return lax.ppermute(x, ("subj", "vox"), moves)


def body(series, offsets, selected):
    devices = lax.axis_size("vox")
    own, keep, give = take_windows(series, offsets, selected)
    taken = swapped(give, 1)
    across = swapped(own, 2)
    beside = swapped(own, 1)
    first = norms(own, beside)
    slab = jnp.concatenate([keep[:KL], taken[:KL], keep[KL:], taken[KL:]], axis=0)
    slab = summed(slab, 8, devices)
    slab = summed(slab, 2, devices)
    beyond = swapped(across, 1)
    mine, theirs = slab[: 2 * KL], slab[2 * KL :]
    ours = along_y(mine, 0, 1, devices)
    left = along_y(theirs, 1, 0, devices)
    right = along_y(theirs, 1, 1, devices)
    second = norms(across, beyond)
    fa = fishers(own, beside, mine, ours, first)
    fb = fishers(across, beyond, left, right, second)
    tiles = partial_kernels(fa, fb, devices)
    tiles = lax.all_to_all(tiles.astype(LINK), "vox", split_axis=0, concat_axis=0, tiled=True)
    tile = jnp.sum(tiles.astype(F32), axis=0)

    def turned(chips):
        moves = [
            (
                j * devices + z * 8 + x * 2 + y,
                ((2 * y + x % 2) ^ (2 * chips)) * devices + z * 8 + (x // 2 * 2 + j % 2) * 2 + j // 2,
            )
            for j in range(GR)
            for z in range(4)
            for x in range(4)
            for y in range(2)
        ]
        return lax.ppermute(tile, ("subj", "vox"), moves)

    here, there = turned(0), turned(1)
    return in_order((here, swapped(here, 1), there, swapped(there, 1)))


def solution(mesh):
    placed = (P("subj", None, "vox"), P(), P())
    return jax.shard_map(
        body, mesh=mesh, in_specs=placed, out_specs=P("vox", "subj", None), check_vma=False
    )
```

```python
import jax
import jax.numpy as jnp
from jax import lax
from jax.experimental import pallas as pl
from jax.experimental.pallas import tpu as pltpu
from jax.sharding import PartitionSpec as P


TR = 16
EP = 12
GR = 4
SL = 4
SB = GR * SL
KL = 16
PART = 2 * SL
HALF = EP * SB // 3
BLOCKS = ((0, 0), (0, 1), (0, 2), (1, 1), (1, 2), (2, 2))
QUARTER = len(BLOCKS) * HALF // GR
VOX = 16384
F32 = jnp.float32
BF16 = jnp.bfloat16
LINK = jnp.float16
series_floor = 1.0
spread_floor = 0.05
shrink_factor = 0.9


def near(x):
    return pltpu.with_memory_space_constraint(x, pltpu.VMEM)


SMEM = pl.BlockSpec(memory_space=pltpu.SMEM)
VMEM = pl.BlockSpec(memory_space=pltpu.VMEM)


def small(mib):
    return pltpu.CompilerParams(vmem_limit_bytes=mib << 20)


def side(h, high):
    return (h + high) % 2


def iota(shape, dim):
    return lax.broadcasted_iota(jnp.int32, shape, dim)


def dot(a, b):
    return jnp.dot(a, b, preferred_element_type=F32)


def dot_nt(a, b):
    return lax.dot_general(a, b, (((1,), (1,)), ((), ())), preferred_element_type=F32)


def split(x):
    hi = x.astype(BF16)
    return hi, (x - hi.astype(F32)).astype(BF16)


def owner(g, p):
    return (p // 2) * 8 + ((p % 2) * 2 + g % 2) * 2 + g // 2


def window_kernel(off_ref, sel_ref, series_ref, e_ref, keep_ref, give_ref, w_ref):
    j = lax.axis_index("subj")
    i = lax.axis_index("vox")
    width = series_ref.shape[2]
    lead = iota((TR, series_ref.shape[1]), 1) - iota((TR, series_ref.shape[1]), 0)
    for s in range(SL):
        for e in range(EP):
            chosen = lead == off_ref[j * SL + s, e]
            w_ref[e * TR : (e + 1) * TR, :] = jnp.where(chosen, 1.0, 0.0).astype(BF16)
        rows = dot(w_ref[...], series_ref[s]).astype(BF16)
        for e in range(EP):
            e_ref[e, s * TR : (s + 1) * TR, :] = rows[e * TR : (e + 1) * TR]
    row = iota((GR * KL, 128), 0)
    column = jnp.zeros((GR * KL, 128), jnp.int32)
    for b, r in enumerate((0, 2, 1, 3)):
        for k in range(KL):
            voxel = sel_ref[2 * owner(j ^ r, k // 2) + k % 2]
            column = jnp.where(row == b * KL + k, voxel - i * width, column)
    lane = iota((GR * KL, 128), 1)
    picker = jnp.concatenate(
        [jnp.where(column == lane + c, 1.0, 0.0).astype(BF16) for c in range(0, width, 128)], axis=1
    )
    picked = dot_nt(picker, e_ref[...].reshape(EP * SL * TR, width)).astype(BF16)
    keep_ref[...] = picked[0 : 2 * KL]
    give_ref[...] = picked[2 * KL :]


def take_windows(series, offsets, selected):
    width = series.shape[2]
    return pl.pallas_call(
        window_kernel,
        out_shape=(
            pltpu.VMEM((EP, SL * TR, width), BF16),
            pltpu.VMEM((2 * KL, EP * SL * TR), BF16),
            pltpu.VMEM((2 * KL, EP * SL * TR), BF16),
        ),
        in_specs=[
            pl.BlockSpec(memory_space=pltpu.SMEM),
            pl.BlockSpec(memory_space=pltpu.SMEM),
            pl.BlockSpec(memory_space=pltpu.VMEM),
        ],
        out_specs=(pl.BlockSpec(memory_space=pltpu.VMEM),) * 3,
        scratch_shapes=[pltpu.VMEM((EP * TR, series.shape[1]), BF16)],
        compiler_params=pltpu.CompilerParams(vmem_limit_bytes=8 << 20),
        name="windows",
    )(
        pltpu.with_memory_space_constraint(offsets, pltpu.HBM),
        pltpu.with_memory_space_constraint(selected, pltpu.HBM),
        pltpu.with_memory_space_constraint(series, pltpu.HBM),
    )


def meeting(j):
    place = iota((PART, 2 * SL * TR), 1)
    home = ((place // TR) % SL) * 2 + ((place // (SL * TR)) ^ j) % 2
    return iota((PART, 2 * SL * TR), 0) == home


def norm_kernel(e0, e1, n_ref):
    gather = jnp.where(meeting(lax.axis_index("subj")), 1.0, 0.0).astype(BF16)
    for e in range(EP):
        x = jnp.concatenate([e0[e], e1[e]], axis=0)
        xf = x.astype(F32)
        high, low = split(xf * xf)
        total = dot(gather, x)
        square = dot(gather, high) + dot(gather, low)
        n_ref[e] = square - total * total * (1.0 / TR)


def norms(e0, e1):
    return pl.pallas_call(
        norm_kernel,
        out_shape=pltpu.VMEM((EP, PART, e0.shape[2]), F32),
        in_specs=[VMEM] * 2,
        out_specs=VMEM,
        compiler_params=small(4),
        name="norms",
    )(near(e0), near(e1))


def fisher_kernel(e0, e1, s0, s1, n_ref, f_ref, l_ref):
    width = e0.shape[2]
    deep = 2 * SL * TR
    chunk = SL * TR
    mine = jnp.where(meeting(lax.axis_index("subj")), 1.0, 0.0)
    mine = jnp.concatenate([mine, mine], axis=0).astype(BF16)
    same = (iota((deep, deep), 0) // TR == iota((deep, deep), 1) // TR).astype(F32).astype(BF16)
    both = (s0[...].astype(F32) + s1[...].astype(F32)).astype(BF16)
    slab = jnp.concatenate(
        [
            jnp.concatenate([both[r : r + KL, e * chunk : (e + 1) * chunk] for r in (0, KL)], axis=1)
            for e in range(EP)
        ],
        axis=0,
    )
    raw = slab.astype(F32)
    high, low = split(raw * raw)
    total = dot(slab, same)
    power = dot(high, same) + dot(low, same) - total * total * (1.0 / TR)
    slab_std = (raw - total * (1.0 / TR)) * (lax.rsqrt(power + series_floor) * shrink_factor)
    high = slab_std.astype(BF16).astype(F32)
    middle = (slab_std - high).astype(BF16).astype(F32)
    thirds = (high, middle, slab_std - high - middle)
    for e in range(EP):
        x = jnp.concatenate([e0[e], e1[e]] * 3, axis=0)
        norm = jnp.sqrt(n_ref[e] + series_floor)[None]
        for k in range(0, KL, 2):
            for n, third in enumerate(thirds):
                row = e * KL + k
                line = [jnp.broadcast_to(third[r : r + 1], (PART, deep)) for r in (row, row + 1)]
                line = jnp.concatenate(line, axis=0).astype(BF16) * mine
                l_ref[e % 2, k * PART : (k + 2) * PART, n * deep : (n + 1) * deep] = line
        shrunk = dot(l_ref[e % 2], x).reshape(KL, PART, width)
        f_ref[e] = jnp.log((norm + shrunk) / (norm - shrunk)).reshape(KL * PART, width)


def fishers(e0, e1, s0, s1, power):
    width = e0.shape[2]
    return pl.pallas_call(
        fisher_kernel,
        out_shape=pltpu.VMEM((EP, KL * PART, width), F32),
        in_specs=[VMEM] * 5,
        out_specs=VMEM,
        scratch_shapes=[pltpu.VMEM((2, KL * PART, 6 * SL * TR), BF16)],
        compiler_params=small(8),
        name="fishers",
    )(*map(near, (e0, e1, s0, s1, power)))


def kernel_kernel(fa, fb, o_ref, z_ref):
    width = fa.shape[2]

    def scores(q, slot):
        for h in range(2):
            rows = pl.ds(pl.multiple_of((q * 2 + h) * PART, PART), PART)
            for c in range(0, width, 128):
                tiles = []
                for f_ref in (fa, fb):
                    fisher = [f_ref[e, rows, c : c + 128] for e in range(EP)]
                    mean = sum(fisher[1:], fisher[0]) * (1.0 / EP)
                    fisher = [f - mean for f in fisher]
                    spread = fisher[0] * fisher[0]
                    for f in fisher[1:]:
                        spread = spread + f * f
                    scale = lax.rsqrt(spread * (1.0 / EP) + 4.0 * spread_floor)
                    tiles.append([f * scale for f in fisher])
                for e in range(EP):
                    at = (e - h * EP // 3) % EP * SB
                    tile = jnp.concatenate([tiles[0][e], tiles[1][e]], axis=0).astype(BF16)
                    z_ref[slot, h, at : at + SB, c : c + 128] = tile

    def products(q, slot):
        for h in range(2):
            product = dot_nt(z_ref[slot, h], z_ref[slot, h])
            for n, (low, high) in enumerate(BLOCKS):
                line, column = ((m - h) % 3 * HALF for m in (low, high))
                tile = product[line : line + HALF, column : column + HALF]
                column = side(h, high) * HALF
                for first in range(0, HALF, HALF // 2):
                    r, line = divmod(n * HALF + first, QUARTER)
                    to = (q // 2) * 8 + (slot * 2 + r % 2) * 2 + r // 2
                    part = tile[first : first + HALF // 2]
                    o_ref[to, line : line + HALF // 2, column : column + HALF] = part

    def step(t, carry):
        products(2 * t, 0)
        scores(2 * t + 1, 1)
        products(2 * t + 1, 1)
        scores(2 * t + 2, 0)
        return carry

    last = KL // 2 - 1
    scores(0, 0)
    lax.fori_loop(0, last // 2, step, 0)
    products(last - 1, 0)
    scores(last, 1)
    products(last, 1)


def partial_kernels(fa, fb, devices):
    width = fa.shape[2]
    return pl.pallas_call(
        kernel_kernel,
        out_shape=pltpu.VMEM((devices, QUARTER, 2 * HALF), F32),
        in_specs=[VMEM] * 2,
        out_specs=VMEM,
        scratch_shapes=[pltpu.VMEM((2, 2, EP * SB, width), BF16)],
        compiler_params=small(8),
        name="partial_kernels",
    )(near(fa), near(fb))


def order_kernel(y0, y1, y2, y3, o_ref, b_ref, k_ref):
    j = lax.axis_index("subj")
    for r, y in enumerate((y0, y1, y2, y3)):
        b_ref[pl.ds(pl.multiple_of((j ^ r) * QUARTER, QUARTER), QUARTER), :] = y[...]
    for n, (low, high) in enumerate(BLOCKS):
        tile = b_ref[n * HALF : (n + 1) * HALF, :]
        mirrored = tile.T
        for h in range(2):
            place = side(h, high) * HALF
            block = tile[:, place : place + HALF]
            at = (high % 2) * HALF
            k_ref[h, high // 2, low * HALF : (low + 1) * HALF, at : at + HALF] = block
            if low != high:
                block = mirrored[place : place + HALF]
                at = (low % 2) * HALF
                k_ref[h, low // 2, high * HALF : (high + 1) * HALF, at : at + HALF] = block
    cols = EP * SB
    turn = lax.axis_index("vox") % 2
    source = iota((cols, cols), 0)
    group = (((source // PART) % 2) ^ turn) * 2 + source % 2
    target = group * (EP * SL) + ((source // 2) % SL) * EP + source // SB
    column = jnp.where(iota((cols, cols), 1) == target, 1.0, 0.0).astype(BF16)
    for h in range(2):
        lines = []
        for s in range(SL):
            own = pl.ds((j // 2 ^ turn) * PART + s * 2 + j % 2, EP, stride=SB)
            lines.append(jnp.concatenate([k_ref[h, 0, own, :], k_ref[h, 1, own, :][:, 0:HALF]], axis=1))
        whole = jnp.concatenate(lines, axis=0)
        high, _ = split(whole)
        middle, low = split(whole - high.astype(F32))
        o_ref[h] = (dot(high, column) + dot(middle, column) + dot(low, column)) * (1.0 / VOX)


def in_order(tiles):
    return pl.pallas_call(
        order_kernel,
        out_shape=jax.ShapeDtypeStruct((2, EP * SL, EP * SB), F32),
        in_specs=[pl.BlockSpec(memory_space=pltpu.VMEM)] * GR,
        out_specs=pl.BlockSpec(memory_space=pltpu.VMEM),
        scratch_shapes=[
            pltpu.VMEM((len(BLOCKS) * HALF, 2 * HALF), F32),
            pltpu.VMEM((2, 2, EP * SB, 2 * HALF), F32),
        ],
        compiler_params=pltpu.CompilerParams(vmem_limit_bytes=4 << 20),
        name="in_order",
    )(*map(near, tiles))


def swapped(x, r):
    return lax.ppermute(x, "subj", [(n, n ^ r) for n in range(GR)])


def summed(x, stride, devices):
    parts = [
        lax.ppermute(x, "vox", [(n, n ^ (step * stride)) for n in range(devices)])
        for step in (1, 3, 2)
    ]
    return sum(parts, x)


def along_y(x, chips, halves, devices):
    moves = [
        (j * devices + i, (j ^ (2 * chips)) * devices + (i ^ halves))
        for j in range(GR)
        for i in range(devices)
    ]
    return lax.ppermute(x, ("subj", "vox"), moves)


def body(series, offsets, selected):
    devices = lax.axis_size("vox")
    own, keep, give = take_windows(series, offsets, selected)
    taken = swapped(give, 1)
    across = swapped(own, 2)
    beside = swapped(own, 1)
    first = norms(own, beside)
    slab = jnp.concatenate([keep[:KL], taken[:KL], keep[KL:], taken[KL:]], axis=0)
    slab = summed(slab, 8, devices)
    slab = summed(slab, 2, devices)
    beyond = swapped(across, 1)
    mine, theirs = slab[: 2 * KL], slab[2 * KL :]
    ours = along_y(mine, 0, 1, devices)
    left = along_y(theirs, 1, 0, devices)
    right = along_y(theirs, 1, 1, devices)
    second = norms(across, beyond)
    fa = fishers(own, beside, mine, ours, first)
    fb = fishers(across, beyond, left, right, second)
    tiles = partial_kernels(fa, fb, devices)
    tiles = lax.all_to_all(tiles.astype(LINK), "vox", split_axis=0, concat_axis=0, tiled=True)
    tile = jnp.sum(tiles.astype(F32), axis=0)

    def turned(chips):
        moves = [
            (
                j * devices + z * 8 + x * 2 + y,
                ((2 * y + x % 2) ^ (2 * chips)) * devices + z * 8 + (x // 2 * 2 + j % 2) * 2 + j // 2,
            )
            for j in range(GR)
            for z in range(4)
            for x in range(4)
            for y in range(2)
        ]
        return lax.ppermute(tile, ("subj", "vox"), moves)

    here, there = turned(0), turned(1)
    return in_order((here, swapped(here, 1), there, swapped(there, 1)))


def solution(mesh):
    placed = (P("subj", None, "vox"), P(), P())
    return jax.shard_map(
        body, mesh=mesh, in_specs=placed, out_specs=P("vox", "subj", None), check_vma=False
    )
```

```python
import jax
import jax.numpy as jnp
from jax import lax
from jax.experimental import pallas as pl
from jax.experimental.pallas import tpu as pltpu
from jax.sharding import PartitionSpec as P


TR = 16
EP = 12
GR = 4
SL = 4
SB = GR * SL
KL = 16
PART = 2 * SL
HALF = EP * SB // 3
UPPER = ((0, 1), (0, 2), (1, 2))
TILES = len(UPPER) + 2
QUARTER = TILES * HALF // GR
VOX = 16384
F32 = jnp.float32
BF16 = jnp.bfloat16
LINK = jnp.float16
series_floor = 1.0
spread_floor = 0.05
shrink_factor = 0.9


def near(x):
    return pltpu.with_memory_space_constraint(x, pltpu.VMEM)


SMEM = pl.BlockSpec(memory_space=pltpu.SMEM)
VMEM = pl.BlockSpec(memory_space=pltpu.VMEM)


def small(mib):
    return pltpu.CompilerParams(vmem_limit_bytes=mib << 20)


def side(h, high):
    return (h + high) % 2


def iota(shape, dim):
    return lax.broadcasted_iota(jnp.int32, shape, dim)


def dot(a, b):
    return jnp.dot(a, b, preferred_element_type=F32)


def dot_nt(a, b):
    return lax.dot_general(a, b, (((1,), (1,)), ((), ())), preferred_element_type=F32)


def split(x):
    hi = x.astype(BF16)
    return hi, (x - hi.astype(F32)).astype(BF16)


def owner(g, p):
    return (p // 2) * 8 + ((p % 2) * 2 + g % 2) * 2 + g // 2


def window_kernel(off_ref, sel_ref, series_ref, e_ref, keep_ref, give_ref, w_ref):
    j = lax.axis_index("subj")
    i = lax.axis_index("vox")
    width = series_ref.shape[2]
    lead = iota((TR, series_ref.shape[1]), 1) - iota((TR, series_ref.shape[1]), 0)
    for s in range(SL):
        for e in range(EP):
            chosen = lead == off_ref[j * SL + s, e]
            w_ref[e * TR : (e + 1) * TR, :] = jnp.where(chosen, 1.0, 0.0).astype(BF16)
        rows = dot(w_ref[...], series_ref[s]).astype(BF16)
        for e in range(EP):
            e_ref[e, s * TR : (s + 1) * TR, :] = rows[e * TR : (e + 1) * TR]
    row = iota((GR * KL, 128), 0)
    column = jnp.zeros((GR * KL, 128), jnp.int32)
    for b, r in enumerate((0, 2, 1, 3)):
        for k in range(KL):
            voxel = sel_ref[2 * owner(j ^ r, k // 2) + k % 2]
            column = jnp.where(row == b * KL + k, voxel - i * width, column)
    lane = iota((GR * KL, 128), 1)
    picker = jnp.concatenate(
        [jnp.where(column == lane + c, 1.0, 0.0).astype(BF16) for c in range(0, width, 128)], axis=1
    )
    picked = dot_nt(picker, e_ref[...].reshape(EP * SL * TR, width)).astype(BF16)
    keep_ref[...] = picked[0 : 2 * KL]
    give_ref[...] = picked[2 * KL :]


def take_windows(series, offsets, selected):
    width = series.shape[2]
    return pl.pallas_call(
        window_kernel,
        out_shape=(
            pltpu.VMEM((EP, SL * TR, width), BF16),
            pltpu.VMEM((2 * KL, EP * SL * TR), BF16),
            pltpu.VMEM((2 * KL, EP * SL * TR), BF16),
        ),
        in_specs=[
            pl.BlockSpec(memory_space=pltpu.SMEM),
            pl.BlockSpec(memory_space=pltpu.SMEM),
            pl.BlockSpec(memory_space=pltpu.VMEM),
        ],
        out_specs=(pl.BlockSpec(memory_space=pltpu.VMEM),) * 3,
        scratch_shapes=[pltpu.VMEM((EP * TR, series.shape[1]), BF16)],
        compiler_params=pltpu.CompilerParams(vmem_limit_bytes=8 << 20),
        name="windows",
    )(
        pltpu.with_memory_space_constraint(offsets, pltpu.HBM),
        pltpu.with_memory_space_constraint(selected, pltpu.HBM),
        pltpu.with_memory_space_constraint(series, pltpu.HBM),
    )


def meeting(j):
    place = iota((PART, 2 * SL * TR), 1)
    home = ((place // TR) % SL) * 2 + ((place // (SL * TR)) ^ j) % 2
    return iota((PART, 2 * SL * TR), 0) == home


def norm_kernel(e0, e1, n_ref):
    gather = jnp.where(meeting(lax.axis_index("subj")), 1.0, 0.0).astype(BF16)
    for e in range(EP):
        x = jnp.concatenate([e0[e], e1[e]], axis=0)
        xf = x.astype(F32)
        high, low = split(xf * xf)
        total = dot(gather, x)
        square = dot(gather, high) + dot(gather, low)
        n_ref[e] = square - total * total * (1.0 / TR)


def norms(e0, e1):
    return pl.pallas_call(
        norm_kernel,
        out_shape=pltpu.VMEM((EP, PART, e0.shape[2]), F32),
        in_specs=[VMEM] * 2,
        out_specs=VMEM,
        compiler_params=small(4),
        name="norms",
    )(near(e0), near(e1))


def fisher_kernel(e0, e1, s0, s1, n_ref, f_ref, l_ref):
    width = e0.shape[2]
    deep = 2 * SL * TR
    chunk = SL * TR
    mine = jnp.where(meeting(lax.axis_index("subj")), 1.0, 0.0)
    mine = jnp.concatenate([mine, mine], axis=0).astype(BF16)
    same = (iota((deep, deep), 0) // TR == iota((deep, deep), 1) // TR).astype(F32).astype(BF16)
    both = (s0[...].astype(F32) + s1[...].astype(F32)).astype(BF16)
    slab = jnp.concatenate(
        [
            jnp.concatenate([both[r : r + KL, e * chunk : (e + 1) * chunk] for r in (0, KL)], axis=1)
            for e in range(EP)
        ],
        axis=0,
    )
    raw = slab.astype(F32)
    high, low = split(raw * raw)
    total = dot(slab, same)
    power = dot(high, same) + dot(low, same) - total * total * (1.0 / TR)
    slab_std = (raw - total * (1.0 / TR)) * (lax.rsqrt(power + series_floor) * shrink_factor)
    high = slab_std.astype(BF16).astype(F32)
    middle = (slab_std - high).astype(BF16).astype(F32)
    thirds = (high, middle, slab_std - high - middle)
    for e in range(EP):
        x = jnp.concatenate([e0[e], e1[e]] * 3, axis=0)
        norm = jnp.sqrt(n_ref[e] + series_floor)[None]
        for k in range(0, KL, 2):
            for n, third in enumerate(thirds):
                row = e * KL + k
                line = [jnp.broadcast_to(third[r : r + 1], (PART, deep)) for r in (row, row + 1)]
                line = jnp.concatenate(line, axis=0).astype(BF16) * mine
                l_ref[e % 2, k * PART : (k + 2) * PART, n * deep : (n + 1) * deep] = line
        shrunk = dot(l_ref[e % 2], x).reshape(KL, PART, width)
        f_ref[e] = jnp.log((norm + shrunk) / (norm - shrunk)).reshape(KL * PART, width)


def fishers(e0, e1, s0, s1, power):
    width = e0.shape[2]
    return pl.pallas_call(
        fisher_kernel,
        out_shape=pltpu.VMEM((EP, KL * PART, width), F32),
        in_specs=[VMEM] * 5,
        out_specs=VMEM,
        scratch_shapes=[pltpu.VMEM((2, KL * PART, 6 * SL * TR), BF16)],
        compiler_params=small(8),
        name="fishers",
    )(*map(near, (e0, e1, s0, s1, power)))


def kernel_kernel(fa, fb, o_ref, z_ref):
    width = fa.shape[2]

    def scores(q, slot):
        for h in range(2):
            rows = pl.ds(pl.multiple_of((q * 2 + h) * PART, PART), PART)
            for c in range(0, width, 128):
                tiles = []
                for f_ref in (fa, fb):
                    fisher = [f_ref[e, rows, c : c + 128] for e in range(EP)]
                    mean = sum(fisher[1:], fisher[0]) * (1.0 / EP)
                    fisher = [f - mean for f in fisher]
                    spread = fisher[0] * fisher[0]
                    for f in fisher[1:]:
                        spread = spread + f * f
                    scale = lax.rsqrt(spread * (1.0 / EP) + 4.0 * spread_floor)
                    tiles.append([f * scale for f in fisher])
                for e in range(EP):
                    at = (e - h * EP // 3) % EP * SB
                    tile = jnp.concatenate([tiles[0][e], tiles[1][e]], axis=0).astype(BF16)
                    z_ref[slot, h, at : at + SB, c : c + 128] = tile

    down, across = iota((HALF, HALF), 0), iota((HALF, HALF), 1)

    def products(q, slot):
        whole = [dot_nt(z_ref[slot, h], z_ref[slot, h]) for h in range(2)]

        def block(h, low, high):
            line, column = ((m - h) % 3 * HALF for m in (low, high))
            return whole[h][line : line + HALF, column : column + HALF]

        tiles = []
        for low, high in UPPER:
            first = side(0, high)
            tiles.append([block(first, low, high), block(1 - first, low, high)])
        mixed, rest = [], jnp.zeros((HALF, HALF), F32)
        for m in range(3):
            second = block(1, m, m)
            mixed.append(jnp.where(across <= down, block(0, m, m), second))
            ends = jnp.sum(jnp.where(across == down, second, 0.0), axis=1, keepdims=True)
            rest = jnp.where(across == m, ends, rest)
        tiles += [mixed[0:2], [mixed[2], rest]]
        for n, tile in enumerate(tiles):
            tile = jnp.concatenate(tile, axis=1)
            for first in range(0, HALF, SB):
                r, line = divmod(n * HALF + first, QUARTER)
                to = (q // 2) * 8 + (slot * 2 + r % 2) * 2 + r // 2
                o_ref[to, line : line + SB, :] = tile[first : first + SB]

    scores(0, 0)
    for q in range(1, KL // 2):
        products(q - 1, (q - 1) % 2)
        scores(q, q % 2)
    products(KL // 2 - 1, 1)


def partial_kernels(fa, fb, devices):
    width = fa.shape[2]
    return pl.pallas_call(
        kernel_kernel,
        out_shape=pltpu.VMEM((devices, QUARTER, 2 * HALF), F32),
        in_specs=[VMEM] * 2,
        out_specs=VMEM,
        scratch_shapes=[pltpu.VMEM((2, 2, EP * SB, width), BF16)],
        compiler_params=small(8),
        name="partial_kernels",
    )(near(fa), near(fb))


def order_kernel(y0, y1, y2, y3, o_ref, b_ref, k_ref):
    j = lax.axis_index("subj")
    for r, y in enumerate((y0, y1, y2, y3)):
        b_ref[pl.ds(pl.multiple_of((j ^ r) * QUARTER, QUARTER), QUARTER), :] = y[...]

    def put(h, low, high, block):
        at = (high % 2) * HALF
        k_ref[h, high // 2, low * HALF : (low + 1) * HALF, at : at + HALF] = block

    down, across = iota((HALF, HALF), 0), iota((HALF, HALF), 1)
    for n in range(TILES):
        tile = b_ref[n * HALF : (n + 1) * HALF, :]
        mirrored = tile.T
        if n < len(UPPER):
            low, high = UPPER[n]
            for h in range(2):
                place = side(h, high) * HALF
                put(h, low, high, tile[:, place : place + HALF])
                put(h, high, low, mirrored[place : place + HALF])
            continue
        for m in range((n - len(UPPER)) * 2, min((n - len(UPPER)) * 2 + 2, 3)):
            place = m % 2 * HALF
            mixed, flipped = tile[:, place : place + HALF], mirrored[place : place + HALF]
            ends = b_ref[(TILES - 1) * HALF : TILES * HALF, HALF + m : HALF + m + 1]
            put(0, m, m, jnp.where(across <= down, mixed, flipped))
            second = jnp.where(across > down, mixed, flipped)
            put(1, m, m, jnp.where(across == down, ends, second))
    cols = EP * SB
    turn = lax.axis_index("vox") % 2
    source = iota((cols, cols), 0)
    group = (((source // PART) % 2) ^ turn) * 2 + source % 2
    target = group * (EP * SL) + ((source // 2) % SL) * EP + source // SB
    column = jnp.where(iota((cols, cols), 1) == target, 1.0, 0.0).astype(BF16)
    for h in range(2):
        lines = []
        for s in range(SL):
            own = pl.ds((j // 2 ^ turn) * PART + s * 2 + j % 2, EP, stride=SB)
            lines.append(jnp.concatenate([k_ref[h, 0, own, :], k_ref[h, 1, own, :][:, 0:HALF]], axis=1))
        whole = jnp.concatenate(lines, axis=0)
        high, _ = split(whole)
        middle, low = split(whole - high.astype(F32))
        o_ref[h] = (dot(high, column) + dot(middle, column) + dot(low, column)) * (1.0 / VOX)


def in_order(tiles):
    return pl.pallas_call(
        order_kernel,
        out_shape=jax.ShapeDtypeStruct((2, EP * SL, EP * SB), F32),
        in_specs=[pl.BlockSpec(memory_space=pltpu.VMEM)] * GR,
        out_specs=pl.BlockSpec(memory_space=pltpu.VMEM),
        scratch_shapes=[
            pltpu.VMEM((TILES * HALF, 2 * HALF), F32),
            pltpu.VMEM((2, 2, EP * SB, 2 * HALF), F32),
        ],
        compiler_params=pltpu.CompilerParams(vmem_limit_bytes=4 << 20),
        name="in_order",
    )(*map(near, tiles))


def swapped(x, r):
    return lax.ppermute(x, "subj", [(n, n ^ r) for n in range(GR)])


def summed(x, stride, devices):
    parts = [
        lax.ppermute(x, "vox", [(n, n ^ (step * stride)) for n in range(devices)])
        for step in (1, 3, 2)
    ]
    return sum(parts, x)


def along_y(x, chips, halves, devices):
    moves = [
        (j * devices + i, (j ^ (2 * chips)) * devices + (i ^ halves))
        for j in range(GR)
        for i in range(devices)
    ]
    return lax.ppermute(x, ("subj", "vox"), moves)


def body(series, offsets, selected):
    devices = lax.axis_size("vox")
    own, keep, give = take_windows(series, offsets, selected)
    taken = swapped(give, 1)
    across = swapped(own, 2)
    beside = swapped(own, 1)
    first = norms(own, beside)
    slab = jnp.concatenate([keep[:KL], taken[:KL], keep[KL:], taken[KL:]], axis=0)
    slab = summed(slab, 8, devices)
    slab = summed(slab, 2, devices)
    beyond = swapped(across, 1)
    mine, theirs = slab[: 2 * KL], slab[2 * KL :]
    ours = along_y(mine, 0, 1, devices)
    left = along_y(theirs, 1, 0, devices)
    right = along_y(theirs, 1, 1, devices)
    second = norms(across, beyond)
    fa = fishers(own, beside, mine, ours, first)
    fb = fishers(across, beyond, left, right, second)
    tiles = partial_kernels(fa, fb, devices)
    tiles = lax.all_to_all(tiles.astype(LINK), "vox", split_axis=0, concat_axis=0, tiled=True)
    tile = jnp.sum(tiles.astype(F32), axis=0)

    def turned(chips):
        moves = [
            (
                j * devices + z * 8 + x * 2 + y,
                ((2 * y + x % 2) ^ (2 * chips)) * devices + z * 8 + (x // 2 * 2 + j % 2) * 2 + j // 2,
            )
            for j in range(GR)
            for z in range(4)
            for x in range(4)
            for y in range(2)
        ]
        return lax.ppermute(tile, ("subj", "vox"), moves)

    here, there = turned(0), turned(1)
    return in_order((here, swapped(here, 1), there, swapped(there, 1)))


def solution(mesh):
    placed = (P("subj", None, "vox"), P(), P())
    return jax.shard_map(
        body, mesh=mesh, in_specs=placed, out_specs=P("vox", "subj", None), check_vma=False
    )
```

```python
import jax
import jax.numpy as jnp
from jax import lax
from jax.experimental import pallas as pl
from jax.experimental.pallas import tpu as pltpu
from jax.sharding import PartitionSpec as P


TR = 16
EP = 12
GR = 4
SL = 4
SB = GR * SL
KL = 16
PART = 2 * SL
HALF = EP * SB // 3
UPPER = ((0, 1), (0, 2), (1, 2))
TILES = len(UPPER) + 2
QUARTER = TILES * HALF // GR
VOX = 16384
F32 = jnp.float32
BF16 = jnp.bfloat16
LINK = jnp.float16
series_floor = 1.0
spread_floor = 0.05
shrink_factor = 0.9


def near(x):
    return pltpu.with_memory_space_constraint(x, pltpu.VMEM)


SMEM = pl.BlockSpec(memory_space=pltpu.SMEM)
VMEM = pl.BlockSpec(memory_space=pltpu.VMEM)


def small(mib):
    return pltpu.CompilerParams(vmem_limit_bytes=mib << 20)


ORDER = (
    31, 23, 30, 22, 10, 21, 7, 24, 17, 0, 15, 14, 1, 19, 5, 13,
    20, 27, 8, 4, 18, 9, 26, 11, 12, 6, 29, 3, 16, 28, 25, 2,
)


def side(h, high):
    return (h + high) % 2


def iota(shape, dim):
    return lax.broadcasted_iota(jnp.int32, shape, dim)


def dot(a, b):
    return jnp.dot(a, b, preferred_element_type=F32)


def dot_nt(a, b):
    return lax.dot_general(a, b, (((1,), (1,)), ((), ())), preferred_element_type=F32)


def split(x):
    hi = x.astype(BF16)
    return hi, (x - hi.astype(F32)).astype(BF16)


def owner(g, p):
    return (p // 2) * 8 + ((p % 2) * 2 + g % 2) * 2 + g // 2


def window_kernel(off_ref, sel_ref, series_ref, e_ref, keep_ref, give_ref, w_ref):
    j = lax.axis_index("subj")
    i = lax.axis_index("vox")
    width = series_ref.shape[2]
    lead = iota((TR, series_ref.shape[1]), 1) - iota((TR, series_ref.shape[1]), 0)
    for s in range(SL):
        for e in range(EP):
            chosen = lead == off_ref[j * SL + s, e]
            w_ref[e * TR : (e + 1) * TR, :] = jnp.where(chosen, 1.0, 0.0).astype(BF16)
        rows = dot(w_ref[...], series_ref[s]).astype(BF16)
        for e in range(EP):
            e_ref[e, s * TR : (s + 1) * TR, :] = rows[e * TR : (e + 1) * TR]
    row = iota((GR * KL, 128), 0)
    column = jnp.zeros((GR * KL, 128), jnp.int32)
    for b, r in enumerate((0, 2, 1, 3)):
        for k in range(KL):
            voxel = sel_ref[2 * owner(j ^ r, k // 2) + k % 2]
            column = jnp.where(row == b * KL + k, voxel - i * width, column)
    lane = iota((GR * KL, 128), 1)
    picker = jnp.concatenate(
        [jnp.where(column == lane + c, 1.0, 0.0).astype(BF16) for c in range(0, width, 128)], axis=1
    )
    picked = dot_nt(picker, e_ref[...].reshape(EP * SL * TR, width)).astype(BF16)
    keep_ref[...] = picked[0 : 2 * KL]
    give_ref[...] = picked[2 * KL :]


def take_windows(series, offsets, selected):
    width = series.shape[2]
    return pl.pallas_call(
        window_kernel,
        out_shape=(
            pltpu.VMEM((EP, SL * TR, width), BF16),
            pltpu.VMEM((2 * KL, EP * SL * TR), BF16),
            pltpu.VMEM((2 * KL, EP * SL * TR), BF16),
        ),
        in_specs=[
            pl.BlockSpec(memory_space=pltpu.SMEM),
            pl.BlockSpec(memory_space=pltpu.SMEM),
            pl.BlockSpec(memory_space=pltpu.VMEM),
        ],
        out_specs=(pl.BlockSpec(memory_space=pltpu.VMEM),) * 3,
        scratch_shapes=[pltpu.VMEM((EP * TR, series.shape[1]), BF16)],
        compiler_params=pltpu.CompilerParams(vmem_limit_bytes=8 << 20),
        name="windows",
    )(
        pltpu.with_memory_space_constraint(offsets, pltpu.HBM),
        pltpu.with_memory_space_constraint(selected, pltpu.HBM),
        pltpu.with_memory_space_constraint(series, pltpu.HBM),
    )


def meeting(j):
    place = iota((PART, 2 * SL * TR), 1)
    home = ((place // TR) % SL) * 2 + ((place // (SL * TR)) ^ j) % 2
    return iota((PART, 2 * SL * TR), 0) == home


def norm_kernel(e0, e1, n_ref):
    gather = jnp.where(meeting(lax.axis_index("subj")), 1.0, 0.0).astype(BF16)
    for e in range(EP):
        x = jnp.concatenate([e0[e], e1[e]], axis=0)
        xf = x.astype(F32)
        high, low = split(xf * xf)
        total = dot(gather, x)
        square = dot(gather, high) + dot(gather, low)
        n_ref[e] = square - total * total * (1.0 / TR)


def norms(e0, e1):
    return pl.pallas_call(
        norm_kernel,
        out_shape=pltpu.VMEM((EP, PART, e0.shape[2]), F32),
        in_specs=[VMEM] * 2,
        out_specs=VMEM,
        compiler_params=small(4),
        name="norms",
    )(near(e0), near(e1))


def fisher_kernel(e0, e1, s0, s1, n_ref, f_ref, l_ref):
    width = e0.shape[2]
    deep = 2 * SL * TR
    chunk = SL * TR
    mine = jnp.where(meeting(lax.axis_index("subj")), 1.0, 0.0)
    mine = jnp.concatenate([mine, mine], axis=0).astype(BF16)
    same = (iota((deep, deep), 0) // TR == iota((deep, deep), 1) // TR).astype(F32).astype(BF16)
    both = (s0[...].astype(F32) + s1[...].astype(F32)).astype(BF16)
    slab = jnp.concatenate(
        [
            jnp.concatenate([both[r : r + KL, e * chunk : (e + 1) * chunk] for r in (0, KL)], axis=1)
            for e in range(EP)
        ],
        axis=0,
    )
    raw = slab.astype(F32)
    high, low = split(raw * raw)
    total = dot(slab, same)
    power = dot(high, same) + dot(low, same) - total * total * (1.0 / TR)
    slab_std = (raw - total * (1.0 / TR)) * (lax.rsqrt(power + series_floor) * shrink_factor)
    high = slab_std.astype(BF16).astype(F32)
    middle = (slab_std - high).astype(BF16).astype(F32)
    thirds = (high, middle, slab_std - high - middle)
    for e in range(EP):
        x = jnp.concatenate([e0[e], e1[e]] * 3, axis=0)
        norm = jnp.sqrt(n_ref[e] + series_floor)[None]
        for k in range(0, KL, 2):
            for n, third in enumerate(thirds):
                row = e * KL + k
                line = [jnp.broadcast_to(third[r : r + 1], (PART, deep)) for r in (row, row + 1)]
                line = jnp.concatenate(line, axis=0).astype(BF16) * mine
                l_ref[e % 2, k * PART : (k + 2) * PART, n * deep : (n + 1) * deep] = line
        shrunk = dot(l_ref[e % 2], x).reshape(KL, PART, width)
        f_ref[e] = jnp.log((norm + shrunk) / (norm - shrunk)).reshape(KL * PART, width)


def fishers(e0, e1, s0, s1, power):
    width = e0.shape[2]
    return pl.pallas_call(
        fisher_kernel,
        out_shape=pltpu.VMEM((EP, KL * PART, width), F32),
        in_specs=[VMEM] * 5,
        out_specs=VMEM,
        scratch_shapes=[pltpu.VMEM((2, KL * PART, 6 * SL * TR), BF16)],
        compiler_params=small(8),
        name="fishers",
    )(*map(near, (e0, e1, s0, s1, power)))


def kernel_kernel(fa, fb, o_ref, z_ref):
    width = fa.shape[2]

    def scores(q, slot):
        for h in range(2):
            rows = pl.ds(pl.multiple_of((q * 2 + h) * PART, PART), PART)
            for c in range(0, width, 128):
                tiles = []
                for f_ref in (fa, fb):
                    fisher = [f_ref[e, rows, c : c + 128] for e in range(EP)]
                    mean = sum(fisher[1:], fisher[0]) * (1.0 / EP)
                    fisher = [f - mean for f in fisher]
                    spread = fisher[0] * fisher[0]
                    for f in fisher[1:]:
                        spread = spread + f * f
                    scale = lax.rsqrt(spread * (1.0 / EP) + 4.0 * spread_floor)
                    tiles.append([f * scale for f in fisher])
                for e in range(EP):
                    at = (e - h * EP // 3) % EP * SB
                    tile = jnp.concatenate([tiles[0][e], tiles[1][e]], axis=0).astype(BF16)
                    z_ref[slot, h, at : at + SB, c : c + 128] = tile

    down, across = iota((HALF, HALF), 0), iota((HALF, HALF), 1)

    def products(q, slot):
        whole = [dot_nt(z_ref[slot, h], z_ref[slot, h]) for h in range(2)]

        def block(h, low, high):
            line, column = ((m - h) % 3 * HALF for m in (low, high))
            return whole[h][line : line + HALF, column : column + HALF]

        tiles = []
        for low, high in UPPER:
            first = side(0, high)
            tiles.append([block(first, low, high), block(1 - first, low, high)])
        mixed, rest = [], jnp.zeros((HALF, HALF), F32)
        for m in range(3):
            second = block(1, m, m)
            mixed.append(jnp.where(across <= down, block(0, m, m), second))
            ends = jnp.sum(jnp.where(across == down, second, 0.0), axis=1, keepdims=True)
            rest = jnp.where(across == m, ends, rest)
        tiles += [mixed[0:2], [mixed[2], rest]]
        for n, tile in enumerate(tiles):
            tile = jnp.concatenate(tile, axis=1)
            for first in range(0, HALF, SB):
                r, line = divmod(n * HALF + first, QUARTER)
                to = (q // 2) * 8 + (slot * 2 + r % 2) * 2 + r // 2
                o_ref[ORDER.index(to), line : line + SB, :] = tile[first : first + SB]

    scores(0, 0)
    for q in range(1, KL // 2):
        products(q - 1, (q - 1) % 2)
        scores(q, q % 2)
    products(KL // 2 - 1, 1)


def partial_kernels(fa, fb, devices):
    width = fa.shape[2]
    return pl.pallas_call(
        kernel_kernel,
        out_shape=pltpu.VMEM((devices, QUARTER, 2 * HALF), F32),
        in_specs=[VMEM] * 2,
        out_specs=VMEM,
        scratch_shapes=[pltpu.VMEM((2, 2, EP * SB, width), BF16)],
        compiler_params=small(8),
        name="partial_kernels",
    )(near(fa), near(fb))


def order_kernel(y0, y1, y2, y3, o_ref, b_ref, k_ref):
    j = lax.axis_index("subj")
    for r, y in enumerate((y0, y1, y2, y3)):
        b_ref[pl.ds(pl.multiple_of((j ^ r) * QUARTER, QUARTER), QUARTER), :] = y[...]

    def put(h, low, high, block):
        at = (high % 2) * HALF
        k_ref[h, high // 2, low * HALF : (low + 1) * HALF, at : at + HALF] = block

    down, across = iota((HALF, HALF), 0), iota((HALF, HALF), 1)
    for n in range(TILES):
        tile = b_ref[n * HALF : (n + 1) * HALF, :]
        mirrored = tile.T
        if n < len(UPPER):
            low, high = UPPER[n]
            for h in range(2):
                place = side(h, high) * HALF
                put(h, low, high, tile[:, place : place + HALF])
                put(h, high, low, mirrored[place : place + HALF])
            continue
        for m in range((n - len(UPPER)) * 2, min((n - len(UPPER)) * 2 + 2, 3)):
            place = m % 2 * HALF
            mixed, flipped = tile[:, place : place + HALF], mirrored[place : place + HALF]
            ends = b_ref[(TILES - 1) * HALF : TILES * HALF, HALF + m : HALF + m + 1]
            put(0, m, m, jnp.where(across <= down, mixed, flipped))
            second = jnp.where(across > down, mixed, flipped)
            put(1, m, m, jnp.where(across == down, ends, second))
    cols = EP * SB
    turn = lax.axis_index("vox") % 2
    source = iota((cols, cols), 0)
    group = (((source // PART) % 2) ^ turn) * 2 + source % 2
    target = group * (EP * SL) + ((source // 2) % SL) * EP + source // SB
    column = jnp.where(iota((cols, cols), 1) == target, 1.0, 0.0).astype(BF16)
    for h in range(2):
        lines = []
        for s in range(SL):
            own = pl.ds((j // 2 ^ turn) * PART + s * 2 + j % 2, EP, stride=SB)
            lines.append(jnp.concatenate([k_ref[h, 0, own, :], k_ref[h, 1, own, :][:, 0:HALF]], axis=1))
        whole = jnp.concatenate(lines, axis=0)
        high, _ = split(whole)
        middle, low = split(whole - high.astype(F32))
        o_ref[h] = (dot(high, column) + dot(middle, column) + dot(low, column)) * (1.0 / VOX)


def in_order(tiles):
    return pl.pallas_call(
        order_kernel,
        out_shape=jax.ShapeDtypeStruct((2, EP * SL, EP * SB), F32),
        in_specs=[pl.BlockSpec(memory_space=pltpu.VMEM)] * GR,
        out_specs=pl.BlockSpec(memory_space=pltpu.VMEM),
        scratch_shapes=[
            pltpu.VMEM((TILES * HALF, 2 * HALF), F32),
            pltpu.VMEM((2, 2, EP * SB, 2 * HALF), F32),
        ],
        compiler_params=pltpu.CompilerParams(vmem_limit_bytes=4 << 20),
        name="in_order",
    )(*map(near, tiles))


def swapped(x, r):
    return lax.ppermute(x, "subj", [(n, n ^ r) for n in range(GR)])


def summed(x, stride, devices):
    parts = [
        lax.ppermute(x, "vox", [(n, n ^ (step * stride)) for n in range(devices)])
        for step in (1, 3, 2)
    ]
    return sum(parts, x)


def along_y(x, chips, halves, devices):
    moves = [
        (j * devices + i, (j ^ (2 * chips)) * devices + (i ^ halves))
        for j in range(GR)
        for i in range(devices)
    ]
    return lax.ppermute(x, ("subj", "vox"), moves)


def body(series, offsets, selected):
    devices = lax.axis_size("vox")
    own, keep, give = take_windows(series, offsets, selected)
    taken = swapped(give, 1)
    across = swapped(own, 2)
    beside = swapped(own, 1)
    first = norms(own, beside)
    slab = jnp.concatenate([keep[:KL], taken[:KL], keep[KL:], taken[KL:]], axis=0)
    slab = summed(slab, 8, devices)
    slab = summed(slab, 2, devices)
    beyond = swapped(across, 1)
    mine, theirs = slab[: 2 * KL], slab[2 * KL :]
    ours = along_y(mine, 0, 1, devices)
    left = along_y(theirs, 1, 0, devices)
    right = along_y(theirs, 1, 1, devices)
    second = norms(across, beyond)
    fa = fishers(own, beside, mine, ours, first)
    fb = fishers(across, beyond, left, right, second)
    tiles = partial_kernels(fa, fb, devices)
    tiles = lax.all_to_all(
        tiles.astype(LINK), "vox", 0, 0, axis_index_groups=[list(ORDER)], tiled=True
    )
    tile = jnp.sum(tiles.astype(F32), axis=0)

    def turned(chips):
        moves = [
            (
                j * devices + z * 8 + x * 2 + y,
                ((2 * y + x % 2) ^ (2 * chips)) * devices + z * 8 + (x // 2 * 2 + j % 2) * 2 + j // 2,
            )
            for j in range(GR)
            for z in range(4)
            for x in range(4)
            for y in range(2)
        ]
        return lax.ppermute(tile, ("subj", "vox"), moves)

    here, there = turned(0), turned(1)
    return in_order((here, swapped(here, 1), there, swapped(there, 1)))


def solution(mesh):
    placed = (P("subj", None, "vox"), P(), P())
    return jax.shard_map(
        body, mesh=mesh, in_specs=placed, out_specs=P("vox", "subj", None), check_vma=False
    )
```

```python
import jax
import jax.numpy as jnp
from jax import lax
from jax.experimental import pallas as pl
from jax.experimental.pallas import tpu as pltpu
from jax.sharding import PartitionSpec as P


TR = 16
EP = 12
GR = 4
SL = 4
SB = GR * SL
KL = 16
PART = 2 * SL
HALF = EP * SB // 3
UPPER = ((0, 1), (0, 2), (1, 2))
TILES = len(UPPER) + 2
QUARTER = TILES * HALF // GR
VOX = 16384
F32 = jnp.float32
BF16 = jnp.bfloat16
LINK = jnp.float16
series_floor = 1.0
spread_floor = 0.05
shrink_factor = 0.9


def near(x):
    return pltpu.with_memory_space_constraint(x, pltpu.VMEM)


SMEM = pl.BlockSpec(memory_space=pltpu.SMEM)
VMEM = pl.BlockSpec(memory_space=pltpu.VMEM)


def small(mib):
    return pltpu.CompilerParams(vmem_limit_bytes=mib << 20)


ORDER = (
    31, 23, 30, 22, 10, 21, 7, 24, 17, 0, 15, 14, 1, 19, 5, 13,
    20, 27, 8, 4, 18, 9, 26, 11, 12, 6, 29, 3, 16, 28, 25, 2,
)


OTHER_ORDER = (
    20, 10, 29, 18, 9, 24, 22, 8, 2, 31, 0, 14, 3, 23, 11, 26,
    7, 28, 5, 16, 27, 30, 25, 15, 4, 1, 17, 19, 13, 6, 21, 12,
)


def side(h, high):
    return (h + high) % 2


def iota(shape, dim):
    return lax.broadcasted_iota(jnp.int32, shape, dim)


def dot(a, b):
    return jnp.dot(a, b, preferred_element_type=F32)


def dot_nt(a, b):
    return lax.dot_general(a, b, (((1,), (1,)), ((), ())), preferred_element_type=F32)


def split(x):
    hi = x.astype(BF16)
    return hi, (x - hi.astype(F32)).astype(BF16)


def owner(g, p):
    return (p // 2) * 8 + ((p % 2) * 2 + g % 2) * 2 + g // 2


def window_kernel(off_ref, sel_ref, series_ref, e_ref, keep_ref, give_ref, w_ref):
    j = lax.axis_index("subj")
    i = lax.axis_index("vox")
    width = series_ref.shape[2]
    lead = iota((TR, series_ref.shape[1]), 1) - iota((TR, series_ref.shape[1]), 0)
    for s in range(SL):
        for e in range(EP):
            chosen = lead == off_ref[j * SL + s, e]
            w_ref[e * TR : (e + 1) * TR, :] = jnp.where(chosen, 1.0, 0.0).astype(BF16)
        rows = dot(w_ref[...], series_ref[s]).astype(BF16)
        for e in range(EP):
            e_ref[e, s * TR : (s + 1) * TR, :] = rows[e * TR : (e + 1) * TR]
    row = iota((GR * KL, 128), 0)
    column = jnp.zeros((GR * KL, 128), jnp.int32)
    for b, r in enumerate((0, 2, 1, 3)):
        for k in range(KL):
            voxel = sel_ref[2 * owner(j ^ r, k // 2) + k % 2]
            column = jnp.where(row == b * KL + k, voxel - i * width, column)
    lane = iota((GR * KL, 128), 1)
    picker = jnp.concatenate(
        [jnp.where(column == lane + c, 1.0, 0.0).astype(BF16) for c in range(0, width, 128)], axis=1
    )
    picked = dot_nt(picker, e_ref[...].reshape(EP * SL * TR, width)).astype(BF16)
    keep_ref[...] = picked[0 : 2 * KL]
    give_ref[...] = picked[2 * KL :]


def take_windows(series, offsets, selected):
    width = series.shape[2]
    return pl.pallas_call(
        window_kernel,
        out_shape=(
            pltpu.VMEM((EP, SL * TR, width), BF16),
            pltpu.VMEM((2 * KL, EP * SL * TR), BF16),
            pltpu.VMEM((2 * KL, EP * SL * TR), BF16),
        ),
        in_specs=[
            pl.BlockSpec(memory_space=pltpu.SMEM),
            pl.BlockSpec(memory_space=pltpu.SMEM),
            pl.BlockSpec(memory_space=pltpu.VMEM),
        ],
        out_specs=(pl.BlockSpec(memory_space=pltpu.VMEM),) * 3,
        scratch_shapes=[pltpu.VMEM((EP * TR, series.shape[1]), BF16)],
        compiler_params=pltpu.CompilerParams(vmem_limit_bytes=8 << 20),
        name="windows",
    )(
        pltpu.with_memory_space_constraint(offsets, pltpu.HBM),
        pltpu.with_memory_space_constraint(selected, pltpu.HBM),
        pltpu.with_memory_space_constraint(series, pltpu.HBM),
    )


def meeting(j):
    place = iota((PART, 2 * SL * TR), 1)
    home = ((place // TR) % SL) * 2 + ((place // (SL * TR)) ^ j) % 2
    return iota((PART, 2 * SL * TR), 0) == home


def norm_kernel(e0, e1, n_ref):
    gather = jnp.where(meeting(lax.axis_index("subj")), 1.0, 0.0).astype(BF16)
    for e in range(EP):
        x = jnp.concatenate([e0[e], e1[e]], axis=0)
        xf = x.astype(F32)
        high, low = split(xf * xf)
        total = dot(gather, x)
        square = dot(gather, high) + dot(gather, low)
        n_ref[e] = square - total * total * (1.0 / TR)


def norms(e0, e1):
    return pl.pallas_call(
        norm_kernel,
        out_shape=pltpu.VMEM((EP, PART, e0.shape[2]), F32),
        in_specs=[VMEM] * 2,
        out_specs=VMEM,
        compiler_params=small(4),
        name="norms",
    )(near(e0), near(e1))


def fisher_kernel(e0, e1, s0, s1, n_ref, f_ref, l_ref):
    width = e0.shape[2]
    deep = 2 * SL * TR
    chunk = SL * TR
    mine = jnp.where(meeting(lax.axis_index("subj")), 1.0, 0.0)
    mine = jnp.concatenate([mine, mine], axis=0).astype(BF16)
    same = (iota((deep, deep), 0) // TR == iota((deep, deep), 1) // TR).astype(F32).astype(BF16)
    both = (s0[...].astype(F32) + s1[...].astype(F32)).astype(BF16)
    slab = jnp.concatenate(
        [
            jnp.concatenate([both[r : r + KL, e * chunk : (e + 1) * chunk] for r in (0, KL)], axis=1)
            for e in range(EP)
        ],
        axis=0,
    )
    raw = slab.astype(F32)
    high, low = split(raw * raw)
    total = dot(slab, same)
    power = dot(high, same) + dot(low, same) - total * total * (1.0 / TR)
    slab_std = (raw - total * (1.0 / TR)) * (lax.rsqrt(power + series_floor) * shrink_factor)
    high = slab_std.astype(BF16).astype(F32)
    middle = (slab_std - high).astype(BF16).astype(F32)
    thirds = (high, middle, slab_std - high - middle)
    for e in range(EP):
        x = jnp.concatenate([e0[e], e1[e]] * 3, axis=0)
        norm = jnp.sqrt(n_ref[e] + series_floor)[None]
        for k in range(0, KL, 2):
            for n, third in enumerate(thirds):
                row = e * KL + k
                line = [jnp.broadcast_to(third[r : r + 1], (PART, deep)) for r in (row, row + 1)]
                line = jnp.concatenate(line, axis=0).astype(BF16) * mine
                l_ref[e % 2, k * PART : (k + 2) * PART, n * deep : (n + 1) * deep] = line
        shrunk = dot(l_ref[e % 2], x).reshape(KL, PART, width)
        f_ref[e] = jnp.log((norm + shrunk) / (norm - shrunk)).reshape(KL * PART, width)


def fishers(e0, e1, s0, s1, power):
    width = e0.shape[2]
    return pl.pallas_call(
        fisher_kernel,
        out_shape=pltpu.VMEM((EP, KL * PART, width), F32),
        in_specs=[VMEM] * 5,
        out_specs=VMEM,
        scratch_shapes=[pltpu.VMEM((2, KL * PART, 6 * SL * TR), BF16)],
        compiler_params=small(8),
        name="fishers",
    )(*map(near, (e0, e1, s0, s1, power)))


def kernel_kernel(fa, fb, o_ref, z_ref):
    width = fa.shape[2]

    def scores(q, slot):
        for h in range(2):
            rows = pl.ds(pl.multiple_of((q * 2 + h) * PART, PART), PART)
            for c in range(0, width, 128):
                tiles = []
                for f_ref in (fa, fb):
                    fisher = [f_ref[e, rows, c : c + 128] for e in range(EP)]
                    mean = sum(fisher[1:], fisher[0]) * (1.0 / EP)
                    fisher = [f - mean for f in fisher]
                    spread = fisher[0] * fisher[0]
                    for f in fisher[1:]:
                        spread = spread + f * f
                    scale = lax.rsqrt(spread * (1.0 / EP) + 4.0 * spread_floor)
                    tiles.append([f * scale for f in fisher])
                for e in range(EP):
                    at = (e - h * EP // 3) % EP * SB
                    tile = jnp.concatenate([tiles[0][e], tiles[1][e]], axis=0).astype(BF16)
                    z_ref[slot, h, at : at + SB, c : c + 128] = tile

    down, across = iota((HALF, HALF), 0), iota((HALF, HALF), 1)
    other_core = lax.axis_index("subj") % 2

    def place_of(to):
        place = ORDER.index(to)
        return place + other_core * (OTHER_ORDER.index(to) - place)

    def products(q, slot):
        whole = [dot_nt(z_ref[slot, h], z_ref[slot, h]) for h in range(2)]

        def block(h, low, high):
            line, column = ((m - h) % 3 * HALF for m in (low, high))
            return whole[h][line : line + HALF, column : column + HALF]

        tiles = []
        for low, high in UPPER:
            first = side(0, high)
            tiles.append([block(first, low, high), block(1 - first, low, high)])
        mixed, rest = [], jnp.zeros((HALF, HALF), F32)
        for m in range(3):
            second = block(1, m, m)
            mixed.append(jnp.where(across <= down, block(0, m, m), second))
            ends = jnp.sum(jnp.where(across == down, second, 0.0), axis=1, keepdims=True)
            rest = jnp.where(across == m, ends, rest)
        tiles += [mixed[0:2], [mixed[2], rest]]
        for n, tile in enumerate(tiles):
            tile = jnp.concatenate(tile, axis=1)
            for first in range(0, HALF, SB):
                r, line = divmod(n * HALF + first, QUARTER)
                to = (q // 2) * 8 + (slot * 2 + r % 2) * 2 + r // 2
                o_ref[place_of(to), line : line + SB, :] = tile[first : first + SB]

    scores(0, 0)
    for q in range(1, KL // 2):
        products(q - 1, (q - 1) % 2)
        scores(q, q % 2)
    products(KL // 2 - 1, 1)


def partial_kernels(fa, fb, devices):
    width = fa.shape[2]
    return pl.pallas_call(
        kernel_kernel,
        out_shape=pltpu.VMEM((devices, QUARTER, 2 * HALF), F32),
        in_specs=[VMEM] * 2,
        out_specs=VMEM,
        scratch_shapes=[pltpu.VMEM((2, 2, EP * SB, width), BF16)],
        compiler_params=small(8),
        name="partial_kernels",
    )(near(fa), near(fb))


def order_kernel(y0, y1, y2, y3, o_ref, b_ref, k_ref):
    j = lax.axis_index("subj")
    for r, y in enumerate((y0, y1, y2, y3)):
        b_ref[pl.ds(pl.multiple_of((j ^ r) * QUARTER, QUARTER), QUARTER), :] = y[...]

    def put(h, low, high, block):
        at = (high % 2) * HALF
        k_ref[h, high // 2, low * HALF : (low + 1) * HALF, at : at + HALF] = block

    down, across = iota((HALF, HALF), 0), iota((HALF, HALF), 1)
    for n in range(TILES):
        tile = b_ref[n * HALF : (n + 1) * HALF, :]
        mirrored = tile.T
        if n < len(UPPER):
            low, high = UPPER[n]
            for h in range(2):
                place = side(h, high) * HALF
                put(h, low, high, tile[:, place : place + HALF])
                put(h, high, low, mirrored[place : place + HALF])
            continue
        for m in range((n - len(UPPER)) * 2, min((n - len(UPPER)) * 2 + 2, 3)):
            place = m % 2 * HALF
            mixed, flipped = tile[:, place : place + HALF], mirrored[place : place + HALF]
            ends = b_ref[(TILES - 1) * HALF : TILES * HALF, HALF + m : HALF + m + 1]
            put(0, m, m, jnp.where(across <= down, mixed, flipped))
            second = jnp.where(across > down, mixed, flipped)
            put(1, m, m, jnp.where(across == down, ends, second))
    cols = EP * SB
    turn = lax.axis_index("vox") % 2
    source = iota((cols, cols), 0)
    group = (((source // PART) % 2) ^ turn) * 2 + source % 2
    target = group * (EP * SL) + ((source // 2) % SL) * EP + source // SB
    column = jnp.where(iota((cols, cols), 1) == target, 1.0, 0.0).astype(BF16)
    for h in range(2):
        lines = []
        for s in range(SL):
            own = pl.ds((j // 2 ^ turn) * PART + s * 2 + j % 2, EP, stride=SB)
            lines.append(jnp.concatenate([k_ref[h, 0, own, :], k_ref[h, 1, own, :][:, 0:HALF]], axis=1))
        whole = jnp.concatenate(lines, axis=0)
        high, _ = split(whole)
        middle, low = split(whole - high.astype(F32))
        o_ref[h] = (dot(high, column) + dot(middle, column) + dot(low, column)) * (1.0 / VOX)


def in_order(tiles):
    return pl.pallas_call(
        order_kernel,
        out_shape=jax.ShapeDtypeStruct((2, EP * SL, EP * SB), F32),
        in_specs=[pl.BlockSpec(memory_space=pltpu.VMEM)] * GR,
        out_specs=pl.BlockSpec(memory_space=pltpu.VMEM),
        scratch_shapes=[
            pltpu.VMEM((TILES * HALF, 2 * HALF), F32),
            pltpu.VMEM((2, 2, EP * SB, 2 * HALF), F32),
        ],
        compiler_params=pltpu.CompilerParams(vmem_limit_bytes=4 << 20),
        name="in_order",
    )(*map(near, tiles))


def swapped(x, r):
    return lax.ppermute(x, "subj", [(n, n ^ r) for n in range(GR)])


def summed(x, stride, devices):
    parts = [
        lax.ppermute(x, "vox", [(n, n ^ (step * stride)) for n in range(devices)])
        for step in (1, 3, 2)
    ]
    return sum(parts, x)


def along_y(x, chips, halves, devices):
    moves = [
        (j * devices + i, (j ^ (2 * chips)) * devices + (i ^ halves))
        for j in range(GR)
        for i in range(devices)
    ]
    return lax.ppermute(x, ("subj", "vox"), moves)


def body(series, offsets, selected):
    devices = lax.axis_size("vox")
    own, keep, give = take_windows(series, offsets, selected)
    taken = swapped(give, 1)
    across = swapped(own, 2)
    beside = swapped(own, 1)
    first = norms(own, beside)
    slab = jnp.concatenate([keep[:KL], taken[:KL], keep[KL:], taken[KL:]], axis=0)
    slab = summed(slab, 8, devices)
    slab = summed(slab, 2, devices)
    beyond = swapped(across, 1)
    mine, theirs = slab[: 2 * KL], slab[2 * KL :]
    ours = along_y(mine, 0, 1, devices)
    left = along_y(theirs, 1, 0, devices)
    right = along_y(theirs, 1, 1, devices)
    second = norms(across, beyond)
    fa = fishers(own, beside, mine, ours, first)
    fb = fishers(across, beyond, left, right, second)
    tiles = partial_kernels(fa, fb, devices)
    groups = [[j * devices + i for i in (ORDER, OTHER_ORDER)[j % 2]] for j in range(GR)]
    tiles = lax.all_to_all(
        tiles.astype(LINK), ("subj", "vox"), 0, 0, axis_index_groups=groups, tiled=True
    )
    tile = jnp.sum(tiles.astype(F32), axis=0)

    def turned(chips):
        moves = [
            (
                j * devices + z * 8 + x * 2 + y,
                ((2 * y + x % 2) ^ (2 * chips)) * devices + z * 8 + (x // 2 * 2 + j % 2) * 2 + j // 2,
            )
            for j in range(GR)
            for z in range(4)
            for x in range(4)
            for y in range(2)
        ]
        return lax.ppermute(tile, ("subj", "vox"), moves)

    here, there = turned(0), turned(1)
    return in_order((here, swapped(here, 1), there, swapped(there, 1)))


def solution(mesh):
    placed = (P("subj", None, "vox"), P(), P())
    return jax.shard_map(
        body, mesh=mesh, in_specs=placed, out_specs=P("vox", "subj", None), check_vma=False
    )
```

```python
import jax
import jax.numpy as jnp
from jax import lax
from jax.experimental import pallas as pl
from jax.experimental.pallas import tpu as pltpu
from jax.sharding import PartitionSpec as P


TR = 16
EP = 12
GR = 4
SL = 4
SB = GR * SL
KL = 16
PART = 2 * SL
HALF = EP * SB // 3
UPPER = ((0, 1), (0, 2), (1, 2))
TILES = len(UPPER) + 2
QUARTER = TILES * HALF // GR
VOX = 16384
F32 = jnp.float32
BF16 = jnp.bfloat16
LINK = jnp.float16
series_floor = 1.0
spread_floor = 0.05
shrink_factor = 0.9


def near(x):
    return pltpu.with_memory_space_constraint(x, pltpu.VMEM)


SMEM = pl.BlockSpec(memory_space=pltpu.SMEM)
VMEM = pl.BlockSpec(memory_space=pltpu.VMEM)


def small(mib):
    return pltpu.CompilerParams(vmem_limit_bytes=mib << 20)


ORDER = (
    31, 23, 30, 22, 10, 21, 7, 24, 17, 0, 15, 14, 1, 19, 5, 13,
    20, 27, 8, 4, 18, 9, 26, 11, 12, 6, 29, 3, 16, 28, 25, 2,
)


OTHER_ORDER = (
    20, 10, 29, 18, 9, 24, 22, 8, 2, 31, 0, 14, 3, 23, 11, 26,
    7, 28, 5, 16, 27, 30, 25, 15, 4, 1, 17, 19, 13, 6, 21, 12,
)


def side(h, high):
    return (h + high) % 2


def iota(shape, dim):
    return lax.broadcasted_iota(jnp.int32, shape, dim)


def dot(a, b):
    return jnp.dot(a, b, preferred_element_type=F32)


def dot_nt(a, b):
    return lax.dot_general(a, b, (((1,), (1,)), ((), ())), preferred_element_type=F32)


def split(x):
    hi = x.astype(BF16)
    return hi, (x - hi.astype(F32)).astype(BF16)


def owner(g, p):
    return (p // 2) * 8 + ((p % 2) * 2 + g % 2) * 2 + g // 2


def window_kernel(off_ref, sel_ref, series_hbm, e_ref, keep_ref, give_ref, w_ref, series_ref, sems):
    j = lax.axis_index("subj")
    i = lax.axis_index("vox")
    width = series_ref.shape[2]
    lead = iota((TR, series_ref.shape[1]), 1) - iota((TR, series_ref.shape[1]), 0)
    copies = [
        pltpu.make_async_copy(series_hbm.at[s], series_ref.at[s], sems.at[s]) for s in range(SL)
    ]
    for copy in copies:
        copy.start()
    row = iota((GR * KL, 128), 0)
    column = jnp.zeros((GR * KL, 128), jnp.int32)
    for b, r in enumerate((0, 2, 1, 3)):
        for k in range(KL):
            voxel = sel_ref[2 * owner(j ^ r, k // 2) + k % 2]
            column = jnp.where(row == b * KL + k, voxel - i * width, column)
    lane = iota((GR * KL, 128), 1)
    picker = jnp.concatenate(
        [jnp.where(column == lane + c, 1.0, 0.0).astype(BF16) for c in range(0, width, 128)], axis=1
    )
    for s in range(SL):
        for e in range(EP):
            chosen = lead == off_ref[j * SL + s, e]
            w_ref[s % 2, e * TR : (e + 1) * TR, :] = jnp.where(chosen, 1.0, 0.0).astype(BF16)
        copies[s].wait()
        rows = dot(w_ref[s % 2], series_ref[s]).astype(BF16)
        for e in range(EP):
            e_ref[e, s * TR : (s + 1) * TR, :] = rows[e * TR : (e + 1) * TR]
    picked = dot_nt(picker, e_ref[...].reshape(EP * SL * TR, width)).astype(BF16)
    keep_ref[...] = picked[0 : 2 * KL]
    give_ref[...] = picked[2 * KL :]


def take_windows(series, offsets, selected):
    width = series.shape[2]
    return pl.pallas_call(
        window_kernel,
        out_shape=(
            pltpu.VMEM((EP, SL * TR, width), BF16),
            pltpu.VMEM((2 * KL, EP * SL * TR), BF16),
            pltpu.VMEM((2 * KL, EP * SL * TR), BF16),
        ),
        in_specs=[
            pl.BlockSpec(memory_space=pltpu.SMEM),
            pl.BlockSpec(memory_space=pltpu.SMEM),
            pl.BlockSpec(memory_space=pltpu.HBM),
        ],
        out_specs=(pl.BlockSpec(memory_space=pltpu.VMEM),) * 3,
        scratch_shapes=[
            pltpu.VMEM((2, EP * TR, series.shape[1]), BF16),
            pltpu.VMEM(series.shape, BF16),
            pltpu.SemaphoreType.DMA((SL,)),
        ],
        compiler_params=pltpu.CompilerParams(vmem_limit_bytes=8 << 20),
        name="windows",
    )(
        pltpu.with_memory_space_constraint(offsets, pltpu.HBM),
        pltpu.with_memory_space_constraint(selected, pltpu.HBM),
        pltpu.with_memory_space_constraint(series, pltpu.HBM),
    )


def meeting(j):
    place = iota((PART, 2 * SL * TR), 1)
    home = ((place // TR) % SL) * 2 + ((place // (SL * TR)) ^ j) % 2
    return iota((PART, 2 * SL * TR), 0) == home


def norm_kernel(e0, e1, n_ref):
    gather = jnp.where(meeting(lax.axis_index("subj")), 1.0, 0.0).astype(BF16)
    for e in range(EP):
        x = jnp.concatenate([e0[e], e1[e]], axis=0)
        xf = x.astype(F32)
        high, low = split(xf * xf)
        total = dot(gather, x)
        square = dot(gather, high) + dot(gather, low)
        n_ref[e] = square - total * total * (1.0 / TR)


def norms(e0, e1):
    return pl.pallas_call(
        norm_kernel,
        out_shape=pltpu.VMEM((EP, PART, e0.shape[2]), F32),
        in_specs=[VMEM] * 2,
        out_specs=VMEM,
        compiler_params=small(4),
        name="norms",
    )(near(e0), near(e1))


def fisher_kernel(e0, e1, s0, s1, n_ref, f_ref, l_ref):
    width = e0.shape[2]
    deep = 2 * SL * TR
    chunk = SL * TR
    mine = jnp.where(meeting(lax.axis_index("subj")), 1.0, 0.0)
    mine = jnp.concatenate([mine, mine], axis=0).astype(BF16)
    same = (iota((deep, deep), 0) // TR == iota((deep, deep), 1) // TR).astype(F32).astype(BF16)
    both = (s0[...].astype(F32) + s1[...].astype(F32)).astype(BF16)
    slab = jnp.concatenate(
        [
            jnp.concatenate([both[r : r + KL, e * chunk : (e + 1) * chunk] for r in (0, KL)], axis=1)
            for e in range(EP)
        ],
        axis=0,
    )
    raw = slab.astype(F32)
    high, low = split(raw * raw)
    total = dot(slab, same)
    power = dot(high, same) + dot(low, same) - total * total * (1.0 / TR)
    slab_std = (raw - total * (1.0 / TR)) * (lax.rsqrt(power + series_floor) * shrink_factor)
    high = slab_std.astype(BF16).astype(F32)
    middle = (slab_std - high).astype(BF16).astype(F32)
    thirds = (high, middle, slab_std - high - middle)
    for e in range(EP):
        x = jnp.concatenate([e0[e], e1[e]] * 3, axis=0)
        norm = jnp.sqrt(n_ref[e] + series_floor)[None]
        for k in range(0, KL, 2):
            for n, third in enumerate(thirds):
                row = e * KL + k
                line = [jnp.broadcast_to(third[r : r + 1], (PART, deep)) for r in (row, row + 1)]
                line = jnp.concatenate(line, axis=0).astype(BF16) * mine
                l_ref[e % 2, k * PART : (k + 2) * PART, n * deep : (n + 1) * deep] = line
        shrunk = dot(l_ref[e % 2], x).reshape(KL, PART, width)
        f_ref[e] = jnp.log((norm + shrunk) / (norm - shrunk)).reshape(KL * PART, width)


def fishers(e0, e1, s0, s1, power):
    width = e0.shape[2]
    return pl.pallas_call(
        fisher_kernel,
        out_shape=pltpu.VMEM((EP, KL * PART, width), F32),
        in_specs=[VMEM] * 5,
        out_specs=VMEM,
        scratch_shapes=[pltpu.VMEM((2, KL * PART, 6 * SL * TR), BF16)],
        compiler_params=small(8),
        name="fishers",
    )(*map(near, (e0, e1, s0, s1, power)))


def kernel_kernel(fa, fb, o_ref, z_ref):
    width = fa.shape[2]

    def scores(q, slot):
        for h in range(2):
            rows = pl.ds(pl.multiple_of((q * 2 + h) * PART, PART), PART)
            for c in range(0, width, 128):
                tiles = []
                for f_ref in (fa, fb):
                    fisher = [f_ref[e, rows, c : c + 128] for e in range(EP)]
                    mean = sum(fisher[1:], fisher[0]) * (1.0 / EP)
                    fisher = [f - mean for f in fisher]
                    spread = fisher[0] * fisher[0]
                    for f in fisher[1:]:
                        spread = spread + f * f
                    scale = lax.rsqrt(spread * (1.0 / EP) + 4.0 * spread_floor)
                    tiles.append([f * scale for f in fisher])
                for e in range(EP):
                    at = (e - h * EP // 3) % EP * SB
                    tile = jnp.concatenate([tiles[0][e], tiles[1][e]], axis=0).astype(BF16)
                    z_ref[slot, h, at : at + SB, c : c + 128] = tile

    down, across = iota((HALF, HALF), 0), iota((HALF, HALF), 1)
    other_core = lax.axis_index("subj") % 2

    def place_of(to):
        place = ORDER.index(to)
        return place + other_core * (OTHER_ORDER.index(to) - place)

    def products(q, slot):
        whole = [dot_nt(z_ref[slot, h], z_ref[slot, h]) for h in range(2)]

        def block(h, low, high):
            line, column = ((m - h) % 3 * HALF for m in (low, high))
            return whole[h][line : line + HALF, column : column + HALF]

        tiles = []
        for low, high in UPPER:
            first = side(0, high)
            tiles.append([block(first, low, high), block(1 - first, low, high)])
        mixed, rest = [], jnp.zeros((HALF, HALF), F32)
        for m in range(3):
            second = block(1, m, m)
            mixed.append(jnp.where(across <= down, block(0, m, m), second))
            ends = jnp.sum(jnp.where(across == down, second, 0.0), axis=1, keepdims=True)
            rest = jnp.where(across == m, ends, rest)
        tiles += [mixed[0:2], [mixed[2], rest]]
        for n, tile in enumerate(tiles):
            tile = jnp.concatenate(tile, axis=1)
            for first in range(0, HALF, SB):
                r, line = divmod(n * HALF + first, QUARTER)
                to = (q // 2) * 8 + (slot * 2 + r % 2) * 2 + r // 2
                o_ref[place_of(to), line : line + SB, :] = tile[first : first + SB]

    scores(0, 0)
    for q in range(1, KL // 2):
        products(q - 1, (q - 1) % 2)
        scores(q, q % 2)
    products(KL // 2 - 1, 1)


def partial_kernels(fa, fb, devices):
    width = fa.shape[2]
    return pl.pallas_call(
        kernel_kernel,
        out_shape=pltpu.VMEM((devices, QUARTER, 2 * HALF), F32),
        in_specs=[VMEM] * 2,
        out_specs=VMEM,
        scratch_shapes=[pltpu.VMEM((2, 2, EP * SB, width), BF16)],
        compiler_params=small(8),
        name="partial_kernels",
    )(near(fa), near(fb))


def order_kernel(y0, y1, y2, y3, o_ref, b_ref, k_ref):
    j = lax.axis_index("subj")
    for r, y in enumerate((y0, y1, y2, y3)):
        b_ref[pl.ds(pl.multiple_of((j ^ r) * QUARTER, QUARTER), QUARTER), :] = y[...]

    def put(h, low, high, block):
        at = (high % 2) * HALF
        k_ref[h, high // 2, low * HALF : (low + 1) * HALF, at : at + HALF] = block

    down, across = iota((HALF, HALF), 0), iota((HALF, HALF), 1)
    for n in range(TILES):
        tile = b_ref[n * HALF : (n + 1) * HALF, :]
        mirrored = tile.T
        if n < len(UPPER):
            low, high = UPPER[n]
            for h in range(2):
                place = side(h, high) * HALF
                put(h, low, high, tile[:, place : place + HALF])
                put(h, high, low, mirrored[place : place + HALF])
            continue
        for m in range((n - len(UPPER)) * 2, min((n - len(UPPER)) * 2 + 2, 3)):
            place = m % 2 * HALF
            mixed, flipped = tile[:, place : place + HALF], mirrored[place : place + HALF]
            ends = b_ref[(TILES - 1) * HALF : TILES * HALF, HALF + m : HALF + m + 1]
            put(0, m, m, jnp.where(across <= down, mixed, flipped))
            second = jnp.where(across > down, mixed, flipped)
            put(1, m, m, jnp.where(across == down, ends, second))
    cols = EP * SB
    turn = lax.axis_index("vox") % 2
    source = iota((cols, cols), 0)
    group = (((source // PART) % 2) ^ turn) * 2 + source % 2
    target = group * (EP * SL) + ((source // 2) % SL) * EP + source // SB
    column = jnp.where(iota((cols, cols), 1) == target, 1.0, 0.0).astype(BF16)
    for h in range(2):
        lines = []
        for s in range(SL):
            own = pl.ds((j // 2 ^ turn) * PART + s * 2 + j % 2, EP, stride=SB)
            lines.append(jnp.concatenate([k_ref[h, 0, own, :], k_ref[h, 1, own, :][:, 0:HALF]], axis=1))
        whole = jnp.concatenate(lines, axis=0)
        high, _ = split(whole)
        middle, low = split(whole - high.astype(F32))
        o_ref[h] = (dot(high, column) + dot(middle, column) + dot(low, column)) * (1.0 / VOX)


def in_order(tiles):
    return pl.pallas_call(
        order_kernel,
        out_shape=jax.ShapeDtypeStruct((2, EP * SL, EP * SB), F32),
        in_specs=[pl.BlockSpec(memory_space=pltpu.VMEM)] * GR,
        out_specs=pl.BlockSpec(memory_space=pltpu.VMEM),
        scratch_shapes=[
            pltpu.VMEM((TILES * HALF, 2 * HALF), F32),
            pltpu.VMEM((2, 2, EP * SB, 2 * HALF), F32),
        ],
        compiler_params=pltpu.CompilerParams(vmem_limit_bytes=4 << 20),
        name="in_order",
    )(*map(near, tiles))


def swapped(x, r):
    return lax.ppermute(x, "subj", [(n, n ^ r) for n in range(GR)])


def summed(x, stride, devices):
    parts = [
        lax.ppermute(x, "vox", [(n, n ^ (step * stride)) for n in range(devices)])
        for step in (1, 3, 2)
    ]
    return sum(parts, x)


def along_y(x, chips, halves, devices):
    moves = [
        (j * devices + i, (j ^ (2 * chips)) * devices + (i ^ halves))
        for j in range(GR)
        for i in range(devices)
    ]
    return lax.ppermute(x, ("subj", "vox"), moves)


def body(series, offsets, selected):
    devices = lax.axis_size("vox")
    own, keep, give = take_windows(series, offsets, selected)
    taken = swapped(give, 1)
    across = swapped(own, 2)
    beside = swapped(own, 1)
    first = norms(own, beside)
    slab = jnp.concatenate([keep[:KL], taken[:KL], keep[KL:], taken[KL:]], axis=0)
    slab = summed(slab, 8, devices)
    slab = summed(slab, 2, devices)
    beyond = swapped(across, 1)
    mine, theirs = slab[: 2 * KL], slab[2 * KL :]
    ours = along_y(mine, 0, 1, devices)
    left = along_y(theirs, 1, 0, devices)
    right = along_y(theirs, 1, 1, devices)
    second = norms(across, beyond)
    fa = fishers(own, beside, mine, ours, first)
    fb = fishers(across, beyond, left, right, second)
    tiles = partial_kernels(fa, fb, devices)
    groups = [[j * devices + i for i in (ORDER, OTHER_ORDER)[j % 2]] for j in range(GR)]
    tiles = lax.all_to_all(
        tiles.astype(LINK), ("subj", "vox"), 0, 0, axis_index_groups=groups, tiled=True
    )
    tile = jnp.sum(tiles.astype(F32), axis=0)

    def turned(chips):
        moves = [
            (
                j * devices + z * 8 + x * 2 + y,
                ((2 * y + x % 2) ^ (2 * chips)) * devices + z * 8 + (x // 2 * 2 + j % 2) * 2 + j // 2,
            )
            for j in range(GR)
            for z in range(4)
            for x in range(4)
            for y in range(2)
        ]
        return lax.ppermute(tile, ("subj", "vox"), moves)

    here, there = turned(0), turned(1)
    return in_order((here, swapped(here, 1), there, swapped(there, 1)))


def solution(mesh):
    placed = (P("subj", None, "vox"), P(), P())
    return jax.shard_map(
        body, mesh=mesh, in_specs=placed, out_specs=P("vox", "subj", None), check_vma=False
    )
```
